256 devices in a mesh: replica: 4 (over y, x), tp: 64 (over z, core).
Axes of the slice: x: 2, y: 2, z: 32, core: 2. Of those that a mesh axis runs over, the one named last changes fastest.
The devices are a block of a 4x8x32 slice.
Arguments:
- hidden_in: bfloat16 [16, 16384], P('replica', 'tp'), parts along dimension 0, may hold values from -60 to 60
- norm_gain: bfloat16 [16384], P('tp'), may hold values from 0.5 to 1.5
- w_qkv: bfloat16 [16384, 9216], P(None, 'tp'), may hold values from -0.046875 to 0.046875
- w_out: bfloat16 [8192, 16384], P('tp'), may hold values from -0.1875 to 0.1875
- key_cache: bfloat16 [16, 8192, 512], P('replica', 'tp'), parts along dimension 0, may hold values from -1200 to 1200
- value_cache: bfloat16 [16, 8192, 512], P('replica', 'tp'), parts along dimension 0, may hold values from -6 to 6
- lengths: int32 [16], P('replica'), parts along dimension 0, may hold values from 4096 to 8192
- positions: int32 [16], P('replica'), parts along dimension 0, may hold values from 0 to 16383
Outputs:
- attn_out: bfloat16 [16, 16384], P('replica', 'tp'), parts along dimension 0
- token_scale: float32 [16], P('replica'), parts along dimension 0
The draws below stay inside these ranges and needn't reach their ends.
There are 4 independent parts, one for each index of `replica`. The reference program is written for one: setup_inputs(seed, part) draws one part's arguments, and reference() takes and returns one part's arrays. A program takes and returns all parts, laid end to end along the dimension named above; an argument that names none is the same for every part. Nothing has to cross between parts.
All inputs are finite; a program needn't handle non-finite values.
Results may differ from the reference program's by a relative error of at most 0.017.
The reference program's roundings to bfloat16 on the way count: a program that leaves them out, or rounds other values in their place, can miss the bound.
Values may be sent and summed in bfloat16 or wider, within the bound.
A program may use at most 128 MiB of HBM per device.

```python
import jax
import jax.numpy as jnp
from jax import lax

D = 16384
QUERY_HEADS = 64
KEY_VALUE_HEADS = 4
HEAD_SIZE = 128
BATCH_SEQUENCES = 4
DEVICE_POSITIONS = 128
CACHE_POSITIONS = 8192
QKVW = 9216


def draw_hidden_in(key, part):
    leading_part, second = jax.random.split(key, 2)
    column = jnp.exp(jax.random.uniform(second, (D,), jnp.float32, 0.0, jnp.log(10.0)))
    values = jnp.clip(jax.random.normal(leading_part, (BATCH_SEQUENCES, D), jnp.float32), -6.0, 6.0) * column[None, :]
    return jnp.clip(values, -60.0, 60.0).astype(jnp.bfloat16)


def draw_key_cache(key, part):
    leading_part = jax.random.fold_in(key, 0)
    offset_start = jnp.clip(jax.random.normal(leading_part, (BATCH_SEQUENCES, CACHE_POSITIONS, KEY_VALUE_HEADS * HEAD_SIZE), jnp.float32), -6.0, 6.0)
    return jnp.clip(offset_start, -1200.0, 1200.0).astype(jnp.bfloat16)


def touch_ends(entries, rng, smallest, high):
    index_at = [jax.random.randint(jax.random.fold_in(rng, axis), (), 0, length) for axis, length in enumerate(entries.shape)]
    longest = entries.shape.index(max(entries.shape))
    next_to = index_at[:longest] + [(index_at[longest] + 1) % entries.shape[longest]] + index_at[longest + 1:]
    return entries.at[tuple(index_at)].set(smallest).at[tuple(next_to)].set(high)


def raised(result, key, source, target, blocks, factor):
    owner, partner = [(jnp.arange(result.shape[axis_at]) // (result.shape[axis_at] // blocks)).reshape([-1 if axis == axis_at else 1 for axis in range(result.ndim)]) for axis_at in (source, target)]
    chosen = jax.random.permutation(key, blocks)[partner]
    strong = (owner == chosen) | (owner == (partner + blocks // 2) % blocks)
    return jnp.where(strong, factor * result, result)


def levels(own_key, dims, pieces, smallest, high):
    factor_of, own = 1.0, jax.random.fold_in(own_key, 6)
    for dim, shards_of in pieces:
        steps = jnp.exp(jax.random.uniform(jax.random.fold_in(own, dim), (shards_of,), jnp.float32, smallest / len(pieces), high / len(pieces)))
        factor_of = factor_of * jnp.repeat(steps, dims[dim] // shards_of).reshape([-1 if axis == dim else 1 for axis in range(len(dims))])
    return factor_of


def gaussian(rng, shape, scale, limit, pieces=(), kind=jnp.bfloat16):
    gain = levels(rng, shape, pieces, -0.22, 0.18) if pieces else 1.0
    values = jax.random.normal(rng, shape, jnp.float32) * scale * gain
    return jnp.minimum(jnp.maximum(values, -limit), limit).astype(kind)


def gaussian_with(own_key, shape, scale, bound, cuts, heavy, kind=jnp.bfloat16):
    drawn = scale * jax.random.normal(own_key, shape, jnp.float32)
    if cuts:
        drawn = drawn * levels(own_key, shape, cuts, -0.22, 0.18)
    return jnp.clip(raised(drawn, jax.random.fold_in(own_key, 3), *heavy), -bound, bound).astype(kind)


def setup_inputs(seed: int = 0, part: int = 0) -> dict:
    keys = jax.random.split(jax.random.key(seed), 9)
    own_keys = jax.random.split(jax.random.fold_in(keys[8], part), 9)
    hidden_in = draw_hidden_in(jax.random.fold_in(jax.random.fold_in(keys[8], part), 71), part)
    norm_gain = jnp.clip(1.0 + 0.1 * jax.random.normal(keys[1], (D,), jnp.float32), 0.5, 1.5).astype(jnp.bfloat16)
    w_qkv = gaussian(keys[2], (D, QKVW), D ** -0.5, 0.046875, ((1, 64),))
    w_out = gaussian_with(keys[3], (QUERY_HEADS * HEAD_SIZE, D), (QUERY_HEADS * HEAD_SIZE) ** -0.5, 0.1875, ((0, 64),), (0, 1, 64, 4.0))
    key_cache = draw_key_cache(jax.random.fold_in(jax.random.fold_in(keys[8], part), 71), part)
    value_cache = gaussian(own_keys[5], (BATCH_SEQUENCES, CACHE_POSITIONS, KEY_VALUE_HEADS * HEAD_SIZE), 1.0, 6.0, ((1, 64),))
    lengths = touch_ends(jax.random.randint(own_keys[6], (BATCH_SEQUENCES,), CACHE_POSITIONS // 2, CACHE_POSITIONS + 1), jax.random.fold_in(own_keys[6], 1), CACHE_POSITIONS // 2, CACHE_POSITIONS).astype(jnp.int32)
    positions = touch_ends(jax.random.randint(own_keys[7], (BATCH_SEQUENCES,), 0, 2 * CACHE_POSITIONS), jax.random.fold_in(own_keys[7], 1), 0, (2 * CACHE_POSITIONS) - 1).astype(jnp.int32)
    return dict(hidden_in=hidden_in, norm_gain=norm_gain, w_qkv=w_qkv, w_out=w_out, key_cache=key_cache, value_cache=value_cache, lengths=lengths, positions=positions)


def apply_rotation(heads, positions):
    half = HEAD_SIZE // 2
    freq = 500000.0 ** (-(jnp.arange(half, dtype=jnp.float32) * 2.0) / HEAD_SIZE)
    angle = positions.astype(jnp.float32)[:, None] * freq[None, :]
    cosine = jnp.cos(angle)[:, None, :]
    sine = jnp.sin(angle)[:, None, :]
    leading_part = heads[..., :half]
    second = heads[..., half:]
    return jnp.concatenate([leading_part * cosine - second * sine, second * cosine + leading_part * sine], axis=-1)

def reference(hidden_in, norm_gain, w_qkv, w_out, key_cache, value_cache, lengths, positions):
    batch_count = hidden_in.shape[0]
    group_count = QUERY_HEADS // KEY_VALUE_HEADS
    block_list = CACHE_POSITIONS // DEVICE_POSITIONS
    query_width = QUERY_HEADS * HEAD_SIZE
    key_width = KEY_VALUE_HEADS * HEAD_SIZE
    inv = 1.0 / HEAD_SIZE ** 0.5
    values = hidden_in.astype(jnp.float32)
    rstd = lax.rsqrt(lax.optimization_barrier(jnp.mean(values * values, axis=-1)) + 1e-05)
    normed = values * norm_gain.astype(jnp.float32)[None, :] * rstd[:, None]
    token_scale = (lax.optimization_barrier(jnp.max(jnp.abs(normed), axis=-1)) + 1e-06) / 448.0
    quant = (normed / token_scale[:, None]).astype(jnp.bfloat16)
    query_key_value = (jnp.dot(quant, w_qkv, preferred_element_type=jnp.float32) * token_scale[:, None]).astype(jnp.bfloat16)
    query_rows = apply_rotation(query_key_value[:, :query_width].astype(jnp.float32).reshape(batch_count, QUERY_HEADS, HEAD_SIZE), positions).astype(jnp.bfloat16)
    latest_key = apply_rotation(query_key_value[:, query_width:query_width + key_width].astype(jnp.float32).reshape(batch_count, KEY_VALUE_HEADS, HEAD_SIZE), positions)
    latest_value = query_key_value[:, query_width + key_width:].astype(jnp.float32).reshape(batch_count, KEY_VALUE_HEADS, HEAD_SIZE)
    grouped_query = query_rows.astype(jnp.float32).reshape(batch_count, KEY_VALUE_HEADS, group_count, HEAD_SIZE)
    key_rows = key_cache.astype(jnp.float32).reshape(batch_count, block_list, DEVICE_POSITIONS, KEY_VALUE_HEADS, HEAD_SIZE)
    value_rows = value_cache.astype(jnp.float32).reshape(batch_count, block_list, DEVICE_POSITIONS, KEY_VALUE_HEADS, HEAD_SIZE)
    scores = jnp.einsum('bgjd,bnpgd->bgjnp', grouped_query, key_rows) * inv
    where_pos = jnp.arange(CACHE_POSITIONS, dtype=jnp.int32).reshape(block_list, DEVICE_POSITIONS)
    valid = (where_pos[None, :, :] < lengths[:, None, None])[:, None, None, :, :]
    block_max = lax.optimization_barrier(jnp.max(jnp.where(valid, scores, -1e+30), axis=-1))
    weights = jnp.where(valid, jnp.exp(scores - block_max[..., None]), 0.0)
    block_sum = lax.optimization_barrier(jnp.sum(weights, axis=-1))
    rounded = lax.optimization_barrier(weights.astype(jnp.bfloat16)).astype(jnp.float32)
    block_out = jnp.einsum('bgjnp,bnpgd->bgjnd', rounded, value_rows)
    top = lax.optimization_barrier(jnp.max(block_max, axis=-1))
    factor = jnp.exp(block_max - top[..., None])
    total = lax.optimization_barrier(jnp.sum(block_sum * factor, axis=-1))
    summed = lax.optimization_barrier(jnp.sum(block_out * factor[..., None], axis=-2))
    score_new = jnp.einsum('bgjd,bgd->bgj', grouped_query, latest_key) * inv
    top_new = jnp.maximum(top, score_new)
    keep = jnp.exp(top - top_new)
    fresh = jnp.exp(score_new - top_new)
    total = total * keep + fresh
    summed = summed * keep[..., None] + fresh[..., None] * latest_value[:, :, None, :]
    att = (summed / total[..., None]).reshape(batch_count, query_width).astype(jnp.bfloat16)
    attn_out = jnp.dot(att, w_out, preferred_element_type=jnp.float32).astype(jnp.bfloat16)
    return (attn_out, token_scale)
```

```python
import functools

import jax
import jax.numpy as jnp
import numpy as np
from jax import lax
from jax.experimental import pallas as pl
from jax.experimental.pallas import tpu as pltpu
from jax.sharding import PartitionSpec as P

QUERY_HEADS = 64
KEY_VALUE_HEADS = 4
HEAD = 128
MESH = pl.DeviceIdType.MESH
F32 = jnp.float32
BF16 = jnp.bfloat16


def sublane():
    return lax.broadcasted_iota(jnp.int32, (8, HEAD), 0)


def half_turn(value):
    return pltpu.roll(value, 4, 0)


def send_all(n, me, source, slots, send_sem, recv_sem):
    half = n // 2

    def push(target):
        pltpu.make_async_remote_copy(
            src_ref=source(target),
            dst_ref=slots.at[me],
            send_sem=send_sem,
            recv_sem=recv_sem,
            device_id={"tp": target},
            device_id_type=MESH,
        ).start()

    push(lax.rem(me + half, n))

    def body(k, _):
        push(lax.rem(me + half - 1 - k, n))
        push(lax.rem(me + half + 1 + k, n))
        return 0

    lax.fori_loop(0, half - 1, body, 0)


def await_bytes(n, slots, sem):
    part = slots.at[pl.ds(0, n - 1)]
    pltpu.make_async_copy(part, part, sem).wait()


def kernel(
    n,
    lengths_ref, positions_ref, freq_ref, hidden_ref, gain_ref, w_qkv_hbm, w_out_hbm, key_hbm, value_hbm,
    out_ref, scale_ref,
    w_qkv, w_out, keys, values,
    mine1, slots1, x_ref, proj_ref, mine2, slots2, q_bf, q_f32, kv_new,
    msg3, slots3, msg4, slots4,
    load_sem, send_sem, recv_sem,
):
    me = lax.axis_index("tp")
    loads = [
        pltpu.make_async_copy(src, dst, load_sem.at[k])
        for k, (src, dst) in enumerate(
            ((w_qkv_hbm, w_qkv), (key_hbm, keys), (value_hbm, values), (w_out_hbm, w_out))
        )
    ]
    for load in loads:
        load.start()

    barrier = pltpu.get_barrier_semaphore()

    def greet(d, _):
        pl.semaphore_signal(barrier, inc=1, device_id={"tp": lax.rem(me + d, n)}, device_id_type=MESH)
        return 0

    lax.fori_loop(1, n, greet, 0)

    sub = sublane()
    upper = sub < 4
    lane = lax.broadcasted_iota(jnp.int32, (8, HEAD), 1)
    token = lax.rem(sub, 4)

    hidden = hidden_ref[...].astype(F32)
    packed = jnp.concatenate([hidden[:, :HEAD], hidden[:, HEAD:]], axis=0).astype(BF16)
    gain = gain_ref[...].astype(F32)
    gain2 = jnp.concatenate([gain[:, :HEAD], gain[:, HEAD:]], axis=0).astype(BF16)
    mine1[0:8, :] = packed
    mine1[8:10, :] = gain2
    slots1[me, 0:8, :] = packed
    slots1[me, 8:10, :] = gain2

    position = jnp.zeros((8, HEAD), F32)
    for b in range(4):
        position = jnp.where(token == b, positions_ref[b].astype(F32), position)
    angle = position * freq_ref[...]
    cosine = jnp.cos(angle)
    sine = jnp.where(lane < HEAD // 2, -jnp.sin(angle), jnp.sin(angle))

    pl.semaphore_wait(barrier, n - 1)

    send_all(n, me, lambda _: mine1, slots1, send_sem.at[0], recv_sem.at[0])
    await_bytes(n, slots1, recv_sem.at[0])

    def gained(s):
        h = slots1[s, 0:8, :].astype(F32)
        g = slots1[s, 8:10, :].astype(F32)
        return h, h * jnp.where(upper, g[0:1, :], g[1:2, :])

    def statistics(s, carry):
        squares, peak = carry
        h, hg = gained(s)
        return squares + h * h, jnp.maximum(peak, jnp.abs(hg))

    squares, peak = lax.fori_loop(
        0, n, statistics, (jnp.zeros((8, HEAD), F32), jnp.zeros((8, HEAD), F32)), unroll=8
    )
    squares = squares + half_turn(squares)
    peak = jnp.maximum(peak, half_turn(peak))
    width = w_qkv.shape[0]
    squares = jnp.broadcast_to(jnp.sum(squares, axis=1, keepdims=True), (8, HEAD))
    peak = jnp.broadcast_to(jnp.max(peak, axis=1, keepdims=True), (8, HEAD))
    rstd = lax.rsqrt(squares / width + 1e-05)
    scale = (peak * rstd + 1e-06) / 448.0
    for b in range(4):
        scale_ref[b] = scale[b, 0]

    def quantize(s, _):
        _, hg = gained(s)
        quant = (hg * rstd) / scale
        x_ref[s] = jnp.concatenate([quant, half_turn(quant)], axis=1).astype(BF16)
        return 0

    lax.fori_loop(0, n, quantize, 0, unroll=8)

    loads[0].wait()
    share = width // n

    def project(s, total):
        rows = pl.ds(pl.multiple_of(s * share, share), share)
        return total + jnp.dot(x_ref[s], w_qkv[rows, :], preferred_element_type=F32)

    columns = w_qkv.shape[1]
    proj = lax.fori_loop(0, n, project, jnp.zeros((8, columns), F32), unroll=8)
    proj_ref[...] = jnp.zeros((8, 2 * HEAD), F32)
    proj_ref[:, :columns] = proj * scale[:, 0:1]
    wide = proj_ref[...]
    turn = lax.rem(me, 8)
    turned = wide
    for k in range(1, 8):
        turned = jnp.where(turn == k, pltpu.roll(wide, 16 * k, 1), turned)
    piece = jnp.where(upper, turned[:, :HEAD], half_turn(turned[:, HEAD:])).astype(BF16)
    mine2[...] = piece
    slots2[me] = piece
    send_all(n, me, lambda _: mine2, slots2, send_sem.at[1], recv_sem.at[1])
    await_bytes(n, slots2, recv_sem.at[1])

    zero = jnp.zeros((8, HEAD), F32)

    def halves(h):
        g, k = h // 9, h % 9
        first = slots2[8 * g + k].astype(F32) if k < 8 else None
        second = slots2[8 * g + k - 1].astype(F32) if k > 0 else None
        return first, second

    def pair(p):
        a0, b0 = halves(2 * p)
        a1, b1 = halves(2 * p + 1)
        low = (a0 if a0 is not None else zero) + (half_turn(b0) if b0 is not None else zero)
        high = (half_turn(a1) if a1 is not None else zero) + (b1 if b1 is not None else zero)
        return jnp.where(upper, low, high)

    def rotated(value):
        return value * cosine + pltpu.roll(value, HEAD // 2, 1) * sine

    for p in range(QUERY_HEADS // 2):
        q = rotated(pair(p)).astype(BF16)
        q_bf[8 * p : 8 * p + 8, :] = q
        q_f32[8 * p : 8 * p + 8, :] = q.astype(F32)
    base = QUERY_HEADS // 2
    for p in range(2):
        kv_new[8 * p : 8 * p + 8, :] = rotated(pair(base + p))
        kv_new[16 + 8 * p : 24 + 8 * p, :] = pair(base + 2 + p)

    inv = 1.0 / HEAD**0.5
    rows = 64
    row_token = lax.rem(lax.broadcasted_iota(jnp.int32, (rows, HEAD), 0), 4)
    place = me * keys.shape[1] + lax.broadcasted_iota(jnp.int32, (rows, HEAD), 1)
    limit = jnp.zeros((rows, HEAD), jnp.int32)
    for b in range(4):
        limit = jnp.where(row_token == b, lengths_ref[b], limit)
    valid = place < limit
    wide_lane = lax.broadcasted_iota(jnp.int32, (rows, HEAD), 1)
    loads[1].wait()
    loads[2].wait()
    for g in range(KEY_VALUE_HEADS):
        q = q_bf[rows * g : rows * g + rows, :]
        heads = slice(HEAD * g, HEAD * g + HEAD)
        scores = jnp.zeros((rows, HEAD), F32)
        for b in range(4):
            part = lax.dot_general(
                q, keys[b, :, heads], (((1,), (1,)), ((), ())), preferred_element_type=F32
            )
            scores = jnp.where(row_token == b, part, scores)
        scores = scores * inv
        top = jnp.max(jnp.where(valid, scores, -1e30), axis=1, keepdims=True)
        weights = jnp.where(valid, jnp.exp(scores - top), 0.0)
        total = jnp.sum(weights, axis=1, keepdims=True)
        rounded = weights.astype(BF16)
        block = jnp.zeros((rows, HEAD), F32)
        for b in range(4):
            part = jnp.dot(rounded, values[b, :, heads], preferred_element_type=F32)
            block = jnp.where(row_token == b, part, block)
        stats = jnp.zeros((rows, HEAD), F32)
        for first, left in ((0, top), (3, total)):
            for k in range(3):
                bits = left.astype(BF16).astype(F32)
                at = 16 * (first + k)
                stats = jnp.where((wide_lane >= at) & (wide_lane < at + 16), bits, stats)
                left = left - bits
        for j in range(rows // 8):
            o = block[8 * j : 8 * j + 8, :]
            t = stats[8 * j : 8 * j + 8, :]
            head = 16 * g + 2 * j
            msg3[head] = jnp.where(upper, o, half_turn(t)).astype(BF16)
            msg3[head + 1] = jnp.where(upper, half_turn(o), t).astype(BF16)
    slots3[me] = msg3[me]
    send_all(n, me, lambda t: msg3.at[t], slots3, send_sem.at[2], recv_sem.at[2])

    def pick(ref, start, index):
        both = ref[pl.ds(pl.multiple_of(start + 8 * (index // 2), 8), 8), :]
        return jnp.where(lax.rem(index, 2) == 1, half_turn(both), both)

    group = me // (QUERY_HEADS // KEY_VALUE_HEADS)
    score_new = jnp.sum(pick(q_f32, 0, me) * pick(kv_new, 0, group), axis=1, keepdims=True) * inv
    score_new = jnp.broadcast_to(score_new, (8, HEAD))
    value_new = pick(kv_new, 16, group)

    spot = lax.broadcasted_iota(jnp.int32, (HEAD, 2 * HEAD), 0)
    side = lax.broadcasted_iota(jnp.int32, (HEAD, 2 * HEAD), 1) // HEAD
    chosen = (spot == 48 * side) | (spot == 48 * side + 16) | (spot == 48 * side + 32)
    spread = jnp.where(chosen, 1.0, 0.0).astype(BF16)
    await_bytes(n, slots3, recv_sem.at[2])
    arrived = slots3[...].reshape(n * 8, HEAD)
    ml = jnp.dot(arrived, spread, preferred_element_type=F32).reshape(n, 8, 2 * HEAD)
    tops = ml[:, :, :HEAD]
    top = half_turn(jnp.max(tops, axis=0))
    summed = jnp.zeros((8, HEAD), F32)
    total = jnp.zeros((8, HEAD), F32)
    for s in range(n):
        factor = jnp.exp(half_turn(tops[s]) - top)
        total = total + half_turn(ml[s, :, HEAD:]) * factor
        summed = summed + slots3[s].astype(F32) * factor
    top_new = jnp.maximum(top, score_new)
    keep = jnp.exp(top - top_new)
    fresh = jnp.exp(score_new - top_new)
    total = total * keep + fresh
    summed = summed * keep + fresh * value_new
    att = jnp.where(upper, summed / total, 0.0).astype(BF16)

    loads[3].wait()
    per = w_out.shape[1] // n
    chunk = 4

    def expand(c, _):
        cols = pl.ds(pl.multiple_of(c * (chunk * per), chunk * per), chunk * per)
        part = jnp.dot(att, w_out[:, cols], preferred_element_type=F32)
        for j in range(chunk):
            left = part[:, j * per : j * per + HEAD]
            right = part[:, j * per + HEAD : (j + 1) * per]
            msg4[c * chunk + j] = jnp.where(upper, left, half_turn(right)).astype(BF16)
        return 0

    lax.fori_loop(0, n // chunk, expand, 0, unroll=4)
    send_all(n, me, lambda t: msg4.at[t], slots4, send_sem.at[3], recv_sem.at[3])
    slots4[me] = msg4[me]
    await_bytes(n, slots4, recv_sem.at[3])

    def gather_sum(s, total):
        return total + slots4[s].astype(F32)

    result = lax.fori_loop(0, n, gather_sum, jnp.zeros((8, HEAD), F32), unroll=8)
    out_ref[:, :HEAD] = result[0:4, :].astype(BF16)
    out_ref[:, HEAD:] = half_turn(result)[0:4, :].astype(BF16)

    await_bytes(n, slots1, send_sem.at[0])
    for k, slots in ((1, slots2), (2, slots3), (3, slots4)):
        await_bytes(n, slots, send_sem.at[k])


def on_device(hidden_in, norm_gain, w_qkv, w_out, key_cache, value_cache, lengths, positions):
    n = lax.axis_size("tp")
    half = HEAD // 2
    freq = np.float32(500000.0 ** (-(np.arange(half, dtype=np.float64) * 2.0) / HEAD))
    freq = jnp.asarray(np.concatenate([freq, freq])[None, :])
    vmem = pl.BlockSpec(memory_space=pltpu.VMEM)
    smem = pl.BlockSpec(memory_space=pltpu.SMEM)
    anywhere = pl.BlockSpec(memory_space=pl.ANY)
    batch = hidden_in.shape[0]
    tile = pltpu.VMEM((n, 8, HEAD), BF16)
    attn_out, token_scale = pl.pallas_call(
        functools.partial(kernel, n),
        out_shape=(
            jax.ShapeDtypeStruct(hidden_in.shape, BF16),
            jax.ShapeDtypeStruct((batch,), F32),
        ),
        in_specs=[smem, smem, vmem, vmem, vmem, anywhere, anywhere, anywhere, anywhere],
        out_specs=(vmem, smem),
        scratch_shapes=[
            pltpu.VMEM(w_qkv.shape, BF16),
            pltpu.VMEM(w_out.shape, BF16),
            pltpu.VMEM(key_cache.shape, BF16),
            pltpu.VMEM(value_cache.shape, BF16),
            pltpu.VMEM((10, HEAD), BF16),
            pltpu.VMEM((n, 10, HEAD), BF16),
            pltpu.VMEM((n, 8, 2 * HEAD), BF16),
            pltpu.VMEM((8, 2 * HEAD), F32),
            pltpu.VMEM((8, HEAD), BF16),
            tile,
            pltpu.VMEM((4 * QUERY_HEADS, HEAD), BF16),
            pltpu.VMEM((4 * QUERY_HEADS, HEAD), F32),
            pltpu.VMEM((32, HEAD), F32),
            tile,
            tile,
            tile,
            tile,
            pltpu.SemaphoreType.DMA((4,)),
            pltpu.SemaphoreType.DMA((4,)),
            pltpu.SemaphoreType.DMA((4,)),
        ],
        compiler_params=pltpu.CompilerParams(collective_id=0, has_side_effects=True),
    )(lengths, positions, freq, hidden_in, norm_gain[None, :], w_qkv, w_out, key_cache, value_cache)
    return attn_out, token_scale


def solution(mesh):
    placed = (
        P("replica", "tp"),
        P("tp"),
        P(None, "tp"),
        P("tp", None),
        P("replica", "tp", None),
        P("replica", "tp", None),
        P("replica"),
        P("replica"),
    )
    return jax.shard_map(
        on_device,
        mesh=mesh,
        in_specs=placed,
        out_specs=(P("replica", "tp"), P("replica")),
        check_vma=False,
    )
```

```python
import functools

import jax
import jax.numpy as jnp
import numpy as np
from jax import lax
from jax.experimental import pallas as pl
from jax.experimental.pallas import tpu as pltpu
from jax.sharding import PartitionSpec as P

QUERY_HEADS = 64
KEY_VALUE_HEADS = 4
HEAD = 128
MESH = pl.DeviceIdType.MESH
F32 = jnp.float32
BF16 = jnp.bfloat16


def sublane():
    return lax.broadcasted_iota(jnp.int32, (8, HEAD), 0)


def half_turn(value):
    return pltpu.roll(value, 4, 0)


def same_core(index, core):
    return {"tp": 2 * index + core}


def send_all(chips, chip, core, pieces, send_sem, recv_sem):
    half = chips // 2

    def push(target):
        for k, (source, landing) in enumerate(pieces):
            pltpu.make_async_remote_copy(
                src_ref=source(target),
                dst_ref=landing,
                send_sem=send_sem.at[k],
                recv_sem=recv_sem.at[k],
                device_id=same_core(target, core),
                device_id_type=MESH,
            ).start()

    push(lax.rem(chip + half, chips))

    def body(k, _):
        push(lax.rem(chip + half - 1 - k, chips))
        push(lax.rem(chip + half + 1 + k, chips))
        return 0

    lax.fori_loop(0, half - 1, body, 0)


def await_bytes(part, sem):
    pltpu.make_async_copy(part, part, sem).wait()


def kernel(
    chips,
    lengths_ref, positions_ref, freq_ref, hidden_ref, gain_ref, w_qkv_hbm, w_out_hbm, key_hbm, value_hbm,
    out_ref, scale_ref,
    w_qkv, w_out, keys, values,
    mine1, mineg, slots1, slotsg, proj_ref, mine2, slots2, q_bf, q_f32, kv_new,
    keep3, give3, got3, msg3, slots3, keep4, give4, got4, msg4, slots4,
    load_sem, send_sem, recv_sem, swap_send, swap_recv,
):
    me = lax.axis_index("tp")
    chip, core = me // 2, lax.rem(me, 2)
    other = 1 - core
    partner = {"tp": me + 1 - 2 * core}

    barrier = pltpu.get_barrier_semaphore()
    pl.semaphore_signal(barrier, inc=1, device_id=partner, device_id_type=MESH)

    def greet(d, _):
        target = same_core(lax.rem(chip + d, chips), core)
        pl.semaphore_signal(barrier, inc=1, device_id=target, device_id_type=MESH)
        return 0

    lax.fori_loop(1, chips, greet, 0)

    def swap(src, dst, k):
        copy = pltpu.make_async_remote_copy(
            src_ref=src,
            dst_ref=dst,
            send_sem=swap_send.at[k],
            recv_sem=swap_recv.at[k],
            device_id=partner,
            device_id_type=MESH,
        )
        copy.start()
        return copy

    sub = sublane()
    upper = sub < 4
    lane = lax.broadcasted_iota(jnp.int32, (8, HEAD), 1)
    token = lax.rem(sub, 4)

    hidden = hidden_ref[...].astype(F32)
    packed = jnp.concatenate([hidden[:, :HEAD], hidden[:, HEAD:]], axis=0).astype(BF16)
    gain = gain_ref[...].astype(F32)
    gain2 = jnp.concatenate([gain[:, :HEAD], gain[:, HEAD:]], axis=0).astype(BF16)
    mine1[...] = packed
    mineg[...] = gain2
    slots1[core, chip] = packed
    slotsg[core, chip] = gain2

    loads = [
        pltpu.make_async_copy(src, dst, load_sem.at[k])
        for k, (src, dst) in enumerate(
            ((w_qkv_hbm, w_qkv), (key_hbm, keys), (value_hbm, values), (w_out_hbm, w_out))
        )
    ]
    for load in loads:
        load.start()

    pl.semaphore_wait(barrier, chips)

    send_all(
        chips, chip, core,
        ((lambda _: mine1, slots1.at[core, chip]), (lambda _: mineg, slotsg.at[core, chip])),
        send_sem.at[0], recv_sem.at[0],
    )

    position = jnp.zeros((8, HEAD), F32)
    for b in range(4):
        position = jnp.where(token == b, positions_ref[b].astype(F32), position)
    angle = position * freq_ref[...]
    cosine = jnp.cos(angle)
    sine = jnp.where(lane < HEAD // 2, -jnp.sin(angle), jnp.sin(angle))

    def rest(slots):
        return slots.at[0, pl.ds(0, chips - 1)]

    await_bytes(rest(slots1), recv_sem.at[0, 0])
    await_bytes(rest(slotsg), recv_sem.at[0, 1])
    swaps = [swap(slots1.at[core], slots1.at[core], 0), swap(slotsg.at[core], slotsg.at[core], 1)]

    def gained(c, s):
        h = slots1[c, s].astype(F32)
        g = slotsg[c, s].astype(F32)
        return h, h * jnp.where(upper, g[0:1, :], g[1:2, :])

    def statistics(c, carry):
        def body(s, carry):
            squares, peak = carry
            h, hg = gained(c, s)
            return squares + h * h, jnp.maximum(peak, jnp.abs(hg))

        return lax.fori_loop(0, chips, body, carry, unroll=8)

    carry = statistics(core, (jnp.zeros((8, HEAD), F32), jnp.zeros((8, HEAD), F32)))
    for copy in swaps:
        copy.wait_recv()
    squares, peak = statistics(other, carry)
    squares = squares + half_turn(squares)
    peak = jnp.maximum(peak, half_turn(peak))
    width = w_qkv.shape[1]
    squares = jnp.broadcast_to(jnp.sum(squares, axis=1, keepdims=True), (8, HEAD))
    peak = jnp.broadcast_to(jnp.max(peak, axis=1, keepdims=True), (8, HEAD))
    rstd = lax.rsqrt(squares / width + 1e-05)
    scale = (peak * rstd + 1e-06) / 448.0
    for b in range(4):
        scale_ref[b] = scale[b, 0]

    loads[0].wait()
    share = width // (2 * chips)

    def project(s, total):
        for c in range(2):
            _, hg = gained(c, s)
            quant = (hg * rstd) / scale
            x = jnp.concatenate([quant, half_turn(quant)], axis=1).astype(BF16)
            rows = pl.ds(pl.multiple_of((2 * s + c) * share, share), share)
            total = total + lax.dot_general(
                x, w_qkv[:, rows], (((1,), (1,)), ((), ())), preferred_element_type=F32
            )
        return total

    columns = w_qkv.shape[0]
    proj = lax.fori_loop(0, chips, project, jnp.zeros((8, columns), F32), unroll=8)
    proj_ref[...] = jnp.zeros((8, 2 * HEAD), F32)
    proj_ref[:, :columns] = proj * scale[:, 0:1]
    wide = proj_ref[...]
    turn = lax.rem(me, 8)
    turned = wide
    for k in range(1, 8):
        turned = jnp.where(turn == k, pltpu.roll(wide, 16 * k, 1), turned)
    piece = jnp.where(upper, turned[:, :HEAD], half_turn(turned[:, HEAD:])).astype(BF16)
    mine2[...] = piece
    slots2[core, chip] = piece
    send_all(
        chips, chip, core, ((lambda _: mine2, slots2.at[core, chip]),), send_sem.at[1], recv_sem.at[1]
    )
    await_bytes(rest(slots2), recv_sem.at[1, 0])
    swaps.append(swap(slots2.at[core], slots2.at[core], 2))
    loads[1].wait()
    loads[2].wait()
    swaps[2].wait_recv()

    zero = jnp.zeros((8, HEAD), F32)

    def arrived2(s):
        return slots2[s % 2, s // 2].astype(F32)

    def halves(h):
        g, k = h // 9, h % 9
        first = arrived2(8 * g + k) if k < 8 else None
        second = arrived2(8 * g + k - 1) if k > 0 else None
        return first, second

    def pair(p):
        a0, b0 = halves(2 * p)
        a1, b1 = halves(2 * p + 1)
        low = (a0 if a0 is not None else zero) + (half_turn(b0) if b0 is not None else zero)
        high = (half_turn(a1) if a1 is not None else zero) + (b1 if b1 is not None else zero)
        return jnp.where(upper, low, high)

    def rotated(value):
        return value * cosine + pltpu.roll(value, HEAD // 2, 1) * sine

    for p in range(QUERY_HEADS // 2):
        q = rotated(pair(p)).astype(BF16)
        q_bf[8 * p : 8 * p + 8, :] = q
        q_f32[8 * p : 8 * p + 8, :] = q.astype(F32)
    base = QUERY_HEADS // 2
    for p in range(2):
        kv_new[8 * p : 8 * p + 8, :] = rotated(pair(base + p))
        kv_new[16 + 8 * p : 24 + 8 * p, :] = pair(base + 2 + p)

    inv = 1.0 / HEAD**0.5
    rows = 64
    row_token = lax.rem(lax.broadcasted_iota(jnp.int32, (rows, HEAD), 0), 4)
    place = me * keys.shape[1] + lax.broadcasted_iota(jnp.int32, (rows, HEAD), 1)
    limit = jnp.zeros((rows, HEAD), jnp.int32)
    for b in range(4):
        limit = jnp.where(row_token == b, lengths_ref[b], limit)
    valid = place < limit
    wide_left = lax.broadcasted_iota(jnp.int32, (rows, HEAD), 1) < HEAD // 2
    even_core = core == 0
    first_swap = len(swaps)
    for g in range(KEY_VALUE_HEADS):
        q = q_bf[rows * g : rows * g + rows, :]
        heads = slice(HEAD * g, HEAD * g + HEAD)
        scores = jnp.zeros((rows, HEAD), F32)
        for b in range(4):
            part = lax.dot_general(
                q, keys[b, :, heads], (((1,), (1,)), ((), ())), preferred_element_type=F32
            )
            scores = jnp.where(row_token == b, part, scores)
        scores = scores * inv
        top = jnp.max(jnp.where(valid, scores, -1e30), axis=1, keepdims=True)
        weights = jnp.where(valid, jnp.exp(scores - top), 0.0)
        total = jnp.sum(weights, axis=1, keepdims=True)
        rounded = weights.astype(BF16)
        block = jnp.zeros((rows, HEAD), F32)
        for b in range(4):
            part = jnp.dot(rounded, values[b, :, heads], preferred_element_type=F32)
            block = jnp.where(row_token == b, part, block)
        stats = jnp.where(wide_left, top, total)
        for j in range(rows // 16):
            at = 4 * g + j
            for k, value in enumerate((block, stats)):
                one, two = value[16 * j : 16 * j + 8, :], value[16 * j + 8 : 16 * j + 16, :]
                evens = jnp.where(upper, one, half_turn(two))
                odds = jnp.where(upper, half_turn(one), two)
                keep3[at, k] = jnp.where(even_core, evens, odds)
                give3[at, k] = jnp.where(even_core, odds, evens)
        part = pl.ds(4 * g, 4)
        swaps.append(swap(give3.at[part], got3.at[part], 3 + g))

    def pick(ref, start, index):
        both = ref[pl.ds(pl.multiple_of(start + 8 * (index // 2), 8), 8), :]
        return jnp.where(lax.rem(index, 2) == 1, half_turn(both), both)

    group = me // (QUERY_HEADS // KEY_VALUE_HEADS)
    score_new = jnp.sum(pick(q_f32, 0, me) * pick(kv_new, 0, group), axis=1, keepdims=True) * inv
    score_new = jnp.broadcast_to(score_new, (8, HEAD))
    value_new = pick(kv_new, 16, group)

    left_half = lane < HEAD // 2

    def both_stats(value):
        turned = pltpu.roll(value, HEAD // 2, 1)
        return jnp.where(left_half, value, turned), jnp.where(left_half, turned, value)

    for g in range(KEY_VALUE_HEADS):
        swaps[first_swap + g].wait_recv()
        for j in range(4):
            at = 4 * g + j
            m0, l0 = both_stats(keep3[at, 1])
            m1, l1 = both_stats(got3[at, 1])
            top = jnp.maximum(m0, m1)
            f0, f1 = jnp.exp(m0 - top), jnp.exp(m1 - top)
            total = l0 * f0 + l1 * f1
            block = keep3[at, 0] * f0 + got3[at, 0] * f1
            stats = zero
            for first, left in ((0, top), (3, total)):
                for k in range(3):
                    bits = left.astype(BF16).astype(F32)
                    here = lane >= 16 * (first + k)
                    stats = jnp.where(here, bits, stats)
                    left = left - bits
            stats = jnp.where(lane >= 96, 0.0, stats)
            msg3[2 * at] = jnp.where(upper, block, half_turn(stats)).astype(BF16)
            msg3[2 * at + 1] = jnp.where(upper, half_turn(block), stats).astype(BF16)
    send_all(
        chips, chip, core, ((lambda t: msg3.at[t], slots3.at[chip]),), send_sem.at[2], recv_sem.at[2]
    )
    slots3[chip] = msg3[chip]

    spot = lax.broadcasted_iota(jnp.int32, (HEAD, 2 * HEAD), 0)
    side = lax.broadcasted_iota(jnp.int32, (HEAD, 2 * HEAD), 1) // HEAD
    chosen = (spot == 48 * side) | (spot == 48 * side + 16) | (spot == 48 * side + 32)
    spread = jnp.where(chosen, 1.0, 0.0).astype(BF16)
    loads[3].wait()
    await_bytes(slots3.at[pl.ds(0, chips - 1)], recv_sem.at[2, 0])
    ml = jnp.dot(slots3[...].reshape(chips * 8, HEAD), spread, preferred_element_type=F32)
    ml = ml.reshape(chips, 8, 2 * HEAD)
    tops = ml[:, :, :HEAD]
    top = half_turn(jnp.max(tops, axis=0))
    summed = zero
    total = zero
    for s in range(chips):
        factor = jnp.exp(half_turn(tops[s]) - top)
        total = total + half_turn(ml[s, :, HEAD:]) * factor
        summed = summed + slots3[s].astype(F32) * factor
    top_new = jnp.maximum(top, score_new)
    keep = jnp.exp(top - top_new)
    fresh = jnp.exp(score_new - top_new)
    total = total * keep + fresh
    summed = summed * keep + fresh * value_new
    att = jnp.where(upper, summed / total, 0.0).astype(BF16)

    per = w_out.shape[1] // (2 * chips)

    def expand(side, dest):
        def body(t, _):
            cols = pl.ds(pl.multiple_of((2 * t + side) * per, per), per)
            part = jnp.dot(att, w_out[:, cols], preferred_element_type=F32)
            dest[t] = jnp.where(upper, part[:, :HEAD], half_turn(part[:, HEAD:]))
            return 0

        lax.fori_loop(0, chips, body, 0, unroll=8)

    expand(other, give4)
    last = swap(give4, got4, 3 + KEY_VALUE_HEADS)
    expand(core, keep4)
    last.wait_recv()

    def merge(t, _):
        msg4[t] = (keep4[t] + got4[t]).astype(BF16)
        return 0

    lax.fori_loop(0, chips, merge, 0, unroll=8)
    send_all(
        chips, chip, core, ((lambda t: msg4.at[t], slots4.at[chip]),), send_sem.at[3], recv_sem.at[3]
    )
    slots4[chip] = msg4[chip]
    await_bytes(slots4.at[pl.ds(0, chips - 1)], recv_sem.at[3, 0])

    def gather_sum(s, total):
        return total + slots4[s].astype(F32)

    result = lax.fori_loop(0, chips, gather_sum, zero, unroll=8)
    out_ref[:, :HEAD] = result[0:4, :].astype(BF16)
    out_ref[:, HEAD:] = half_turn(result)[0:4, :].astype(BF16)

    await_bytes(rest(slots1), send_sem.at[0, 0])
    await_bytes(rest(slotsg), send_sem.at[0, 1])
    await_bytes(rest(slots2), send_sem.at[1, 0])
    await_bytes(slots3.at[pl.ds(0, chips - 1)], send_sem.at[2, 0])
    await_bytes(slots4.at[pl.ds(0, chips - 1)], send_sem.at[3, 0])
    for copy in (*swaps, last):
        copy.wait_send()


def on_device(hidden_in, norm_gain, w_qkv, w_out, key_cache, value_cache, lengths, positions):
    chips = lax.axis_size("tp") // 2
    half = HEAD // 2
    freq = np.float32(500000.0 ** (-(np.arange(half, dtype=np.float64) * 2.0) / HEAD))
    freq = jnp.asarray(np.concatenate([freq, freq])[None, :])
    vmem = pl.BlockSpec(memory_space=pltpu.VMEM)
    smem = pl.BlockSpec(memory_space=pltpu.SMEM)
    anywhere = pl.BlockSpec(memory_space=pl.ANY)
    batch = hidden_in.shape[0]
    tiles = pltpu.VMEM((chips, 8, HEAD), BF16)
    tiles_f32 = pltpu.VMEM((chips, 8, HEAD), F32)
    stats = pltpu.VMEM((chips // 2, 2, 8, HEAD), F32)
    attn_out, token_scale = pl.pallas_call(
        functools.partial(kernel, chips),
        out_shape=(
            jax.ShapeDtypeStruct(hidden_in.shape, BF16),
            jax.ShapeDtypeStruct((batch,), F32),
        ),
        in_specs=[smem, smem, vmem, vmem, vmem, anywhere, anywhere, anywhere, anywhere],
        out_specs=(vmem, smem),
        scratch_shapes=[
            pltpu.VMEM(w_qkv.shape[::-1], BF16),
            pltpu.VMEM(w_out.shape, BF16),
            pltpu.VMEM(key_cache.shape, BF16),
            pltpu.VMEM(value_cache.shape, BF16),
            pltpu.VMEM((8, HEAD), BF16),
            pltpu.VMEM((2, HEAD), BF16),
            pltpu.VMEM((2, chips, 8, HEAD), BF16),
            pltpu.VMEM((2, chips, 2, HEAD), BF16),
            pltpu.VMEM((8, 2 * HEAD), F32),
            pltpu.VMEM((8, HEAD), BF16),
            pltpu.VMEM((2, chips, 8, HEAD), BF16),
            pltpu.VMEM((4 * QUERY_HEADS, HEAD), BF16),
            pltpu.VMEM((4 * QUERY_HEADS, HEAD), F32),
            pltpu.VMEM((32, HEAD), F32),
            stats,
            stats,
            stats,
            tiles,
            tiles,
            tiles_f32,
            tiles_f32,
            tiles_f32,
            tiles,
            tiles,
            pltpu.SemaphoreType.DMA((4,)),
            pltpu.SemaphoreType.DMA((4, 2)),
            pltpu.SemaphoreType.DMA((4, 2)),
            pltpu.SemaphoreType.DMA((4 + KEY_VALUE_HEADS,)),
            pltpu.SemaphoreType.DMA((4 + KEY_VALUE_HEADS,)),
        ],
        compiler_params=pltpu.CompilerParams(collective_id=0, has_side_effects=True),
    )(lengths, positions, freq, hidden_in, norm_gain[None, :], w_qkv.T, w_out, key_cache, value_cache)
    return attn_out, token_scale


def solution(mesh):
    placed = (
        P("replica", "tp"),
        P("tp"),
        P(None, "tp"),
        P("tp", None),
        P("replica", "tp", None),
        P("replica", "tp", None),
        P("replica"),
        P("replica"),
    )
    return jax.shard_map(
        on_device,
        mesh=mesh,
        in_specs=placed,
        out_specs=(P("replica", "tp"), P("replica")),
        check_vma=False,
    )
```

```python
import functools

import jax
import jax.numpy as jnp
import numpy as np
from jax import lax
from jax.experimental import pallas as pl
from jax.experimental.pallas import tpu as pltpu
from jax.sharding import PartitionSpec as P

QUERY_HEADS = 64
KEY_VALUE_HEADS = 4
HEAD = 128
MESH = pl.DeviceIdType.MESH
F32 = jnp.float32
BF16 = jnp.bfloat16


def sublane():
    return lax.broadcasted_iota(jnp.int32, (8, HEAD), 0)


def half_turn(value):
    return pltpu.roll(value, 4, 0)


def same_core(index, core):
    return {"tp": 2 * index + core}


def remote(src, dst, send_sem, recv_sem, target):
    copy = pltpu.make_async_remote_copy(
        src_ref=src,
        dst_ref=dst,
        send_sem=send_sem,
        recv_sem=recv_sem,
        device_id=target,
        device_id_type=MESH,
    )
    copy.start()
    return copy


def await_bytes(part, sem):
    pltpu.make_async_copy(part, part, sem).wait()


def kernel(
    chips,
    lengths_hbm, positions_hbm, freq_hbm, hidden_hbm, gain_hbm, w_qkv_hbm, w_out_hbm, key_hbm, value_hbm,
    out_ref, scale_ref,
    w_qkv, w_out, keys, values, lengths_ref, positions_ref, freq_ref, hidden_ref, gain_ref,
    mine1, mineg, slots1, slotsg, proj_ref, mine2, slots2, q_bf, q_f32, kv_new,
    keep3, give3, got3, msg3, slots3, keep4, give4, got4, msg4, slots4,
    load_sem, send_sem, near_sem, recv_sem, swap_send, swap_recv,
):
    me = lax.axis_index("tp")
    chip, core = me // 2, lax.rem(me, 2)
    other = 1 - core
    partner = {"tp": me + 1 - 2 * core}
    reach = chips // 4

    def ahead(d):
        return lax.rem(chip + d + chips, chips)

    barrier = pltpu.get_barrier_semaphore()
    for d in range(reach, 0, -1):
        for target in (ahead(d), ahead(-d)):
            pl.semaphore_signal(
                barrier, inc=1, device_id=same_core(target, core), device_id_type=MESH
            )
    pl.semaphore_signal(barrier, inc=1, device_id=partner, device_id_type=MESH)

    loads = [
        pltpu.make_async_copy(src, dst, load_sem.at[k])
        for k, (src, dst) in enumerate((
            (hidden_hbm, hidden_ref), (gain_hbm, gain_ref), (freq_hbm, freq_ref),
            (positions_hbm, positions_ref), (lengths_hbm, lengths_ref),
            (w_qkv_hbm, w_qkv), (key_hbm, keys), (value_hbm, values), (w_out_hbm, w_out),
        ))
    ]
    for load in loads:
        load.start()

    def swap(src, dst, k):
        return remote(src, dst, swap_send.at[k], swap_recv.at[k], partner)

    sub = sublane()
    upper = sub < 4
    lane = lax.broadcasted_iota(jnp.int32, (8, HEAD), 1)
    token = lax.rem(sub, 4)
    zero = jnp.zeros((8, HEAD), F32)

    loads[0].wait()
    hidden = hidden_ref[...].astype(F32)
    packed = jnp.concatenate([hidden[:, :HEAD], hidden[:, HEAD:]], axis=0).astype(BF16)
    mine1[...] = packed
    slots1[core, chip] = packed
    loads[1].wait()
    gain2 = gain_ref[...].reshape(2, HEAD)
    mineg[...] = gain2
    slotsg[core, chip] = gain2

    pl.semaphore_wait(barrier, 2 * reach + 1)

    parts = ((slots1, mine1), (slotsg, mineg))

    def pace(d):
        return (d - 1) // 2

    for d in range(reach, 0, -1):
        for side in range(2):
            for k, (slots, mine) in enumerate(parts):
                remote(
                    mine, slots.at[core, chip], send_sem.at[0, k], near_sem.at[side, pace(d), k],
                    same_core(ahead(d - 2 * d * side), core),
                )

    loads[2].wait()
    loads[3].wait()
    loads[4].wait()
    position = zero
    for b in range(4):
        position = jnp.where(token == b, positions_ref[b].astype(F32), position)
    angle = position * freq_ref[...]
    cosine = jnp.cos(angle)
    sine = jnp.where(lane < HEAD // 2, -jnp.sin(angle), jnp.sin(angle))

    def rows_of(slots, count):
        return slots.at[0, pl.ds(0, count)]

    for step in range(pace(reach) + 1):
        for side in range(2):
            for k, (slots, _) in enumerate(parts):
                await_bytes(rows_of(slots, 2), near_sem.at[side, step, k])
            for d in (2 * step + 2, 2 * step + 1):
                if d == reach and side == 1:
                    continue
                source = ahead(2 * d * side - d)
                for k, (slots, _) in enumerate(parts):
                    block = slots.at[core, source]
                    remote(
                        block, block, send_sem.at[0, k], recv_sem.at[0, k],
                        same_core(ahead(reach - 2 * reach * side), core),
                    )
    for k, (slots, _) in enumerate(parts):
        await_bytes(rows_of(slots, 2 * reach - 1), recv_sem.at[0, k])
    swaps = [swap(slots1.at[core], slots1.at[core], 0), swap(slotsg.at[core], slotsg.at[core], 1)]

    def gained(c, s):
        h = slots1[c, s].astype(F32)
        g = slotsg[c, s].astype(F32)
        return h, h * jnp.where(upper, g[0:1, :], g[1:2, :])

    def statistics(c, carry):
        def body(s, carry):
            squares, peak = carry
            h, hg = gained(c, s)
            return squares + h * h, jnp.maximum(peak, jnp.abs(hg))

        return lax.fori_loop(0, chips, body, carry, unroll=8)

    carry = statistics(core, (zero, zero))
    for copy in swaps:
        copy.wait_recv()
    squares, peak = statistics(other, carry)
    squares = squares + half_turn(squares)
    peak = jnp.maximum(peak, half_turn(peak))
    width = w_qkv.shape[1]
    squares = jnp.broadcast_to(jnp.sum(squares, axis=1, keepdims=True), (8, HEAD))
    peak = jnp.broadcast_to(jnp.max(peak, axis=1, keepdims=True), (8, HEAD))
    rstd = lax.rsqrt(squares / width + 1e-05)
    scale = (peak * rstd + 1e-06) / 448.0
    for b in range(4):
        scale_ref[b] = scale[b, 0]

    loads[5].wait()
    share = width // (2 * chips)

    def project(s, total):
        for c in range(2):
            _, hg = gained(c, s)
            quant = (hg * rstd) / scale
            x = jnp.concatenate([quant, half_turn(quant)], axis=1).astype(BF16)
            rows = pl.ds(pl.multiple_of((2 * s + c) * share, share), share)
            total = total + lax.dot_general(
                x, w_qkv[:, rows], (((1,), (1,)), ((), ())), preferred_element_type=F32
            )
        return total

    columns = w_qkv.shape[0]
    proj = lax.fori_loop(0, chips, project, jnp.zeros((8, columns), F32), unroll=8)
    proj_ref[...] = jnp.zeros((8, 2 * HEAD), F32)
    proj_ref[:, :columns] = proj * scale[:, 0:1]
    wide = proj_ref[...]
    turn = lax.rem(me, 8)
    turned = wide
    for k in range(1, 8):
        turned = jnp.where(turn == k, pltpu.roll(wide, 16 * k, 1), turned)
    piece = jnp.where(upper, turned[:, :HEAD], half_turn(turned[:, HEAD:])).astype(BF16)
    mine2[...] = piece
    slots2[core, chip] = piece
    half = chips // 2
    far = half - chips // 8
    own2 = slots2.at[core, chip]
    for d in range(half, far, -1):
        for side in range(1 if d == half else 2):
            target = ahead(d - 2 * d * side)
            for c in (core, other):
                remote(mine2, own2, send_sem.at[1, 1], recv_sem.at[1, 1], same_core(target, c))
    for d in range(far, 0, -1):
        for side in range(2):
            remote(
                mine2, own2, send_sem.at[1, 0], recv_sem.at[1, 0],
                same_core(ahead(d - 2 * d * side), core),
            )
    remote(mine2, own2, swap_send.at[2], swap_recv.at[2], partner)
    await_bytes(rows_of(slots2, 2 * far), recv_sem.at[1, 0])
    for d in range(1, far + 1):
        for side in range(2):
            block = slots2.at[core, ahead(d - 2 * d * side)]
            remote(block, block, swap_send.at[2], swap_recv.at[2], partner)
    loads[6].wait()
    loads[7].wait()
    beyond = 2 * (half - far) - 1
    await_bytes(rows_of(slots2, 2 * beyond), recv_sem.at[1, 1])
    await_bytes(rows_of(slots2, 2 * far + 1), swap_recv.at[2])

    def arrived2(s):
        return slots2[s % 2, s // 2].astype(F32)

    def halves(h):
        g, k = h // 9, h % 9
        first = arrived2(8 * g + k) if k < 8 else None
        second = arrived2(8 * g + k - 1) if k > 0 else None
        return first, second

    def pair(p):
        a0, b0 = halves(2 * p)
        a1, b1 = halves(2 * p + 1)
        low = (a0 if a0 is not None else zero) + (half_turn(b0) if b0 is not None else zero)
        high = (half_turn(a1) if a1 is not None else zero) + (b1 if b1 is not None else zero)
        return jnp.where(upper, low, high)

    def rotated(value):
        return value * cosine + pltpu.roll(value, HEAD // 2, 1) * sine

    for p in range(QUERY_HEADS // 2):
        q = rotated(pair(p)).astype(BF16)
        q_bf[8 * p : 8 * p + 8, :] = q
        q_f32[8 * p : 8 * p + 8, :] = q.astype(F32)
    base = QUERY_HEADS // 2
    for p in range(2):
        kv_new[8 * p : 8 * p + 8, :] = rotated(pair(base + p))
        kv_new[16 + 8 * p : 24 + 8 * p, :] = pair(base + 2 + p)

    inv = 1.0 / HEAD**0.5
    rows = 64
    row_token = lax.rem(lax.broadcasted_iota(jnp.int32, (rows, HEAD), 0), 4)
    place = me * keys.shape[1] + lax.broadcasted_iota(jnp.int32, (rows, HEAD), 1)
    limit = jnp.zeros((rows, HEAD), jnp.int32)
    for b in range(4):
        limit = jnp.where(row_token == b, lengths_ref[b], limit)
    valid = place < limit
    wide_left = lax.broadcasted_iota(jnp.int32, (rows, HEAD), 1) < HEAD // 2
    even_core = core == 0
    home = me // (QUERY_HEADS // KEY_VALUE_HEADS)
    order = [lax.rem(home + k, KEY_VALUE_HEADS) for k in (2, 1, 3, 0)]

    def attend(k):
        g = order[k]
        q = q_bf[pl.ds(pl.multiple_of(rows * g, rows), rows), :]
        heads = pl.ds(pl.multiple_of(HEAD * g, HEAD), HEAD)
        scores = jnp.zeros((rows, HEAD), F32)
        for b in range(4):
            part = lax.dot_general(
                q, keys[b, :, heads], (((1,), (1,)), ((), ())), preferred_element_type=F32
            )
            scores = jnp.where(row_token == b, part, scores)
        scores = scores * inv
        top = jnp.max(jnp.where(valid, scores, -1e30), axis=1, keepdims=True)
        weights = jnp.where(valid, jnp.exp(scores - top), 0.0)
        total = jnp.sum(weights, axis=1, keepdims=True)
        rounded = weights.astype(BF16)
        block = jnp.zeros((rows, HEAD), F32)
        for b in range(4):
            part = jnp.dot(rounded, values[b, :, heads], preferred_element_type=F32)
            block = jnp.where(row_token == b, part, block)
        stats = jnp.where(wide_left, top, total)
        for j in range(rows // 16):
            for i, value in enumerate((block, stats)):
                one, two = value[16 * j : 16 * j + 8, :], value[16 * j + 8 : 16 * j + 16, :]
                evens = jnp.where(upper, one, half_turn(two))
                odds = jnp.where(upper, half_turn(one), two)
                keep3[4 * k + j, i] = jnp.where(even_core, evens, odds)
                give3[4 * k + j, i] = jnp.where(even_core, odds, evens)
        part = pl.ds(4 * k, 4)
        return swap(give3.at[part], got3.at[part], 3 + k)

    left_half = lane < HEAD // 2

    def both_stats(value):
        turned = pltpu.roll(value, HEAD // 2, 1)
        return jnp.where(left_half, value, turned), jnp.where(left_half, turned, value)

    def settle(k, copy):
        copy.wait_recv()
        for j in range(4):
            at = 4 * k + j
            m0, l0 = both_stats(keep3[at, 1])
            m1, l1 = both_stats(got3[at, 1])
            top = jnp.maximum(m0, m1)
            f0, f1 = jnp.exp(m0 - top), jnp.exp(m1 - top)
            total = l0 * f0 + l1 * f1
            block = keep3[at, 0] * f0 + got3[at, 0] * f1
            stats = zero
            for first, left in ((0, top), (3, total)):
                for i in range(3):
                    bits = left.astype(BF16).astype(F32)
                    stats = jnp.where(lane >= 16 * (first + i), bits, stats)
                    left = left - bits
            stats = jnp.where(lane >= 96, 0.0, stats)
            msg3[2 * at] = jnp.where(upper, block, half_turn(stats)).astype(BF16)
            msg3[2 * at + 1] = jnp.where(upper, half_turn(block), stats).astype(BF16)
        for i in range(8):
            target = 8 * order[k] + i

            def push():
                remote(
                    msg3.at[8 * k + i], slots3.at[chip], send_sem.at[2, 0], recv_sem.at[2, 0],
                    same_core(target, core),
                )

            if k < 3:
                push()
            else:
                pl.when(target != chip)(push)

    copies = []
    for k in range(KEY_VALUE_HEADS):
        copies.append(attend(k))
        if k >= 2:
            settle(k - 2, copies[k - 2])
    settle(2, copies[2])
    settle(3, copies[3])
    slots3[chip] = msg3[24 + lax.rem(chip, 8)]
    swaps.extend(copies)

    def pick(ref, start, index):
        both = ref[pl.ds(pl.multiple_of(start + 8 * (index // 2), 8), 8), :]
        return jnp.where(lax.rem(index, 2) == 1, half_turn(both), both)

    score_new = jnp.sum(pick(q_f32, 0, me) * pick(kv_new, 0, home), axis=1, keepdims=True) * inv
    score_new = jnp.broadcast_to(score_new, (8, HEAD))
    value_new = pick(kv_new, 16, home)

    spot = lax.broadcasted_iota(jnp.int32, (HEAD, 2 * HEAD), 0)
    side = lax.broadcasted_iota(jnp.int32, (HEAD, 2 * HEAD), 1) // HEAD
    chosen = (spot == 48 * side) | (spot == 48 * side + 16) | (spot == 48 * side + 32)
    spread = jnp.where(chosen, 1.0, 0.0).astype(BF16)
    loads[8].wait()
    await_bytes(slots3.at[pl.ds(0, chips - 1)], recv_sem.at[2, 0])
    ml = jnp.dot(slots3[...].reshape(chips * 8, HEAD), spread, preferred_element_type=F32)
    ml = ml.reshape(chips, 8, 2 * HEAD)
    tops = ml[:, :, :HEAD]
    top = half_turn(jnp.max(tops, axis=0))
    summed = zero
    total = zero
    for s in range(chips):
        factor = jnp.exp(half_turn(tops[s]) - top)
        total = total + half_turn(ml[s, :, HEAD:]) * factor
        summed = summed + slots3[s].astype(F32) * factor
    top_new = jnp.maximum(top, score_new)
    keep = jnp.exp(top - top_new)
    fresh = jnp.exp(score_new - top_new)
    total = total * keep + fresh
    summed = summed * keep + fresh * value_new
    att = jnp.where(upper, summed / total, 0.0).astype(BF16)

    per = w_out.shape[1] // (2 * chips)

    def destination(i):
        return ahead(half + ((i + 1) // 2) * (1 - 2 * lax.rem(i, 2)))

    batches, batch = 4, chips // 4

    def expand(side, dest, first):
        for i in range(first, first + batch):
            cols = pl.ds(pl.multiple_of((2 * destination(i) + side) * per, per), per)
            part = jnp.dot(att, w_out[:, cols], preferred_element_type=F32)
            dest[i] = jnp.where(upper, part[:, :HEAD], half_turn(part[:, HEAD:]))

    copies = []
    for k in range(batches):
        expand(other, give4, batch * k)
        part = pl.ds(batch * k, batch)
        copies.append(swap(give4.at[part], got4.at[part], 3 + KEY_VALUE_HEADS + k))
    swaps.extend(copies)
    for k in range(batches):
        expand(core, keep4, batch * k)
    for k in range(batches):
        copies[k].wait_recv()
        indices = range(batch * k, batch * k + batch)
        for i in indices:
            msg4[i] = (keep4[i] + got4[i]).astype(BF16)
        for i in indices:
            if i < chips - 1:
                remote(
                    msg4.at[i], slots4.at[chip], send_sem.at[3, 0], recv_sem.at[3, 0],
                    same_core(destination(i), core),
                )
    slots4[chip] = msg4[chips - 1]
    await_bytes(slots4.at[pl.ds(0, chips - 1)], recv_sem.at[3, 0])

    def gather_sum(s, total):
        return total + slots4[s].astype(F32)

    result = lax.fori_loop(0, chips, gather_sum, zero, unroll=8)
    out_ref[:, :HEAD] = result[0:4, :].astype(BF16)
    out_ref[:, HEAD:] = half_turn(result)[0:4, :].astype(BF16)

    for k, (slots, _) in enumerate(parts):
        await_bytes(rows_of(slots, chips - 1), send_sem.at[0, k])
    await_bytes(rows_of(slots2, 2 * far), send_sem.at[1, 0])
    await_bytes(rows_of(slots2, 2 * beyond), send_sem.at[1, 1])
    await_bytes(rows_of(slots2, 2 * far + 1), swap_send.at[2])
    await_bytes(slots3.at[pl.ds(0, chips - 1)], send_sem.at[2, 0])
    await_bytes(slots4.at[pl.ds(0, chips - 1)], send_sem.at[3, 0])
    for copy in swaps:
        copy.wait_send()


def on_device(hidden_in, norm_gain, w_qkv, w_out, key_cache, value_cache, lengths, positions):
    chips = lax.axis_size("tp") // 2
    half = HEAD // 2
    freq = np.float32(500000.0 ** (-(np.arange(half, dtype=np.float64) * 2.0) / HEAD))
    freq = jnp.asarray(np.concatenate([freq, freq])[None, :])
    vmem = pl.BlockSpec(memory_space=pltpu.VMEM)
    smem = pl.BlockSpec(memory_space=pltpu.SMEM)
    anywhere = pl.BlockSpec(memory_space=pl.ANY)
    batch = hidden_in.shape[0]
    tiles = pltpu.VMEM((chips, 8, HEAD), BF16)
    tiles_f32 = pltpu.VMEM((chips, 8, HEAD), F32)
    stats = pltpu.VMEM((chips // 2, 2, 8, HEAD), F32)
    attn_out, token_scale = pl.pallas_call(
        functools.partial(kernel, chips),
        out_shape=(
            jax.ShapeDtypeStruct(hidden_in.shape, BF16),
            jax.ShapeDtypeStruct((batch,), F32),
        ),
        in_specs=[anywhere] * 9,
        out_specs=(vmem, smem),
        scratch_shapes=[
            pltpu.VMEM(w_qkv.shape[::-1], BF16),
            pltpu.VMEM(w_out.shape, BF16),
            pltpu.VMEM(key_cache.shape, BF16),
            pltpu.VMEM(value_cache.shape, BF16),
            pltpu.SMEM(lengths.shape, jnp.int32),
            pltpu.SMEM(positions.shape, jnp.int32),
            pltpu.VMEM(freq.shape, F32),
            pltpu.VMEM(hidden_in.shape, BF16),
            pltpu.VMEM(norm_gain.shape, BF16),
            pltpu.VMEM((8, HEAD), BF16),
            pltpu.VMEM((2, HEAD), BF16),
            pltpu.VMEM((2, chips, 8, HEAD), BF16),
            pltpu.VMEM((2, chips, 2, HEAD), BF16),
            pltpu.VMEM((8, 2 * HEAD), F32),
            pltpu.VMEM((8, HEAD), BF16),
            pltpu.VMEM((2, chips, 8, HEAD), BF16),
            pltpu.VMEM((4 * QUERY_HEADS, HEAD), BF16),
            pltpu.VMEM((4 * QUERY_HEADS, HEAD), F32),
            pltpu.VMEM((32, HEAD), F32),
            stats,
            stats,
            stats,
            tiles,
            tiles,
            tiles_f32,
            tiles_f32,
            tiles_f32,
            tiles,
            tiles,
            pltpu.SemaphoreType.DMA((9,)),
            pltpu.SemaphoreType.DMA((4, 2)),
            pltpu.SemaphoreType.DMA((2, chips // 8, 2)),
            pltpu.SemaphoreType.DMA((4, 2)),
            pltpu.SemaphoreType.DMA((7 + KEY_VALUE_HEADS,)),
            pltpu.SemaphoreType.DMA((7 + KEY_VALUE_HEADS,)),
        ],
        compiler_params=pltpu.CompilerParams(collective_id=0, has_side_effects=True),
    )(lengths, positions, freq, hidden_in, norm_gain, w_qkv.T, w_out, key_cache, value_cache)
    return attn_out, token_scale


def solution(mesh):
    placed = (
        P("replica", "tp"),
        P("tp"),
        P(None, "tp"),
        P("tp", None),
        P("replica", "tp", None),
        P("replica", "tp", None),
        P("replica"),
        P("replica"),
    )
    return jax.shard_map(
        on_device,
        mesh=mesh,
        in_specs=placed,
        out_specs=(P("replica", "tp"), P("replica")),
        check_vma=False,
    )
```

```python
import functools

import jax
import jax.numpy as jnp
import numpy as np
from jax import lax
from jax.experimental import pallas as pl
from jax.experimental.pallas import tpu as pltpu
from jax.sharding import PartitionSpec as P

QUERY_HEADS = 64
KEY_VALUE_HEADS = 4
HEAD = 128
MESH = pl.DeviceIdType.MESH
F32 = jnp.float32
BF16 = jnp.bfloat16


def sublane():
    return lax.broadcasted_iota(jnp.int32, (8, HEAD), 0)


def half_turn(value):
    return pltpu.roll(value, 4, 0)


def same_core(index, core):
    return {"tp": 2 * index + core}


def remote(src, dst, send_sem, recv_sem, target):
    copy = pltpu.make_async_remote_copy(
        src_ref=src,
        dst_ref=dst,
        send_sem=send_sem,
        recv_sem=recv_sem,
        device_id=target,
        device_id_type=MESH,
    )
    copy.start()
    return copy


def await_bytes(part, sem):
    pltpu.make_async_copy(part, part, sem).wait()


def kernel(
    chips,
    lengths_hbm, positions_hbm, freq_hbm, hidden_hbm, gain_hbm, w_qkv_hbm, w_out_hbm, key_hbm, value_hbm,
    out_ref, scale_ref,
    w_qkv, w_out, keys, values, lengths_ref, positions_ref, freq_ref, hidden_ref, gain_ref,
    mine1, mineg, slots1, slotsg, x_ref, proj_ref, mine2, slots2, q_bf, q_f32, kv_new,
    keep3, give3, got3, msg3, slots3, keep4, give4, got4, msg4, slots4,
    load_sem, send_sem, near_sem, cross_sem, recv_sem, swap_send, swap_recv,
):
    me = lax.axis_index("tp")
    chip, core = me // 2, lax.rem(me, 2)
    other = 1 - core
    partner = {"tp": me + 1 - 2 * core}
    reach = chips // 4

    def ahead(d):
        return lax.rem(chip + d + chips, chips)

    barrier = pltpu.get_barrier_semaphore()
    for d in range(reach, 0, -1):
        for target in (ahead(d), ahead(-d)):
            for c in (core, other):
                pl.semaphore_signal(
                    barrier, inc=1, device_id=same_core(target, c), device_id_type=MESH
                )
    pl.semaphore_signal(barrier, inc=1, device_id=partner, device_id_type=MESH)

    loads = [
        pltpu.make_async_copy(src, dst, load_sem.at[k])
        for k, (src, dst) in enumerate((
            (hidden_hbm, hidden_ref), (gain_hbm, gain_ref), (freq_hbm, freq_ref),
            (positions_hbm, positions_ref), (lengths_hbm, lengths_ref),
            (w_qkv_hbm, w_qkv), (key_hbm, keys), (value_hbm, values), (w_out_hbm, w_out),
        ))
    ]
    for load in loads:
        load.start()

    def swap(src, dst, k):
        return remote(src, dst, swap_send.at[k], swap_recv.at[k], partner)

    sub = sublane()
    upper = sub < 4
    lane = lax.broadcasted_iota(jnp.int32, (8, HEAD), 1)
    token = lax.rem(sub, 4)
    zero = jnp.zeros((8, HEAD), F32)

    loads[0].wait()
    hidden = hidden_ref[...].astype(F32)
    packed = jnp.concatenate([hidden[:, :HEAD], hidden[:, HEAD:]], axis=0).astype(BF16)
    mine1[...] = packed
    slots1[core, chip] = packed
    loads[1].wait()
    gain2 = gain_ref[...].reshape(2, HEAD)
    mineg[...] = gain2
    slotsg[core, chip] = gain2

    pl.semaphore_wait(barrier, 4 * reach + 1)

    def pace(d):
        return (d - 1) // 2

    def deliver(hidden, gain, source, target, hidden_sem, gain_sem):
        peer = same_core(target, core)
        remote(hidden, slots1.at[core, source], send_sem.at[0, 0], hidden_sem, peer)
        remote(gain, slotsg.at[core, source], send_sem.at[0, 1], gain_sem, peer)
        remote(
            gain, slotsg.at[core, source], send_sem.at[0, 1], cross_sem.at[0], same_core(target, other)
        )

    def pass_on(source):
        block = slots1.at[core, source]
        remote(block, block, swap_send.at[0], swap_recv.at[0], partner)

    for d in range(reach, 0, -1):
        for side in range(2):
            deliver(
                mine1, mineg, chip, ahead(d - 2 * d * side),
                near_sem.at[side, pace(d), 0], near_sem.at[side, pace(d), 1],
            )
    remote(mine1, slots1.at[core, chip], swap_send.at[0], swap_recv.at[0], partner)
    remote(mineg, slotsg.at[core, chip], swap_send.at[1], cross_sem.at[0], partner)

    loads[2].wait()
    loads[3].wait()
    loads[4].wait()
    position = zero
    for b in range(4):
        position = jnp.where(token == b, positions_ref[b].astype(F32), position)
    angle = position * freq_ref[...]
    cosine = jnp.cos(angle)
    sine = jnp.where(lane < HEAD // 2, -jnp.sin(angle), jnp.sin(angle))

    def rows_of(slots, count):
        return slots.at[0, pl.ds(0, count)]

    last_step = pace(reach)
    for step in range(last_step + 1):
        for side in range(2):
            await_bytes(rows_of(slots1, 2), near_sem.at[side, step, 0])
            await_bytes(rows_of(slotsg, 2), near_sem.at[side, step, 1])
            for d in (2 * step + 2, 2 * step + 1):
                if d == reach and side == 1:
                    continue
                source = ahead(2 * d * side - d)
                target = ahead(reach - 2 * reach * side)
                arrival = recv_sem.at[0, 0] if step < last_step else cross_sem.at[1]
                deliver(
                    slots1.at[core, source], slotsg.at[core, source], source, target,
                    arrival, recv_sem.at[0, 1],
                )
                if step == last_step:
                    block = slots1.at[core, source]
                    remote(block, block, send_sem.at[0, 0], cross_sem.at[1], same_core(target, other))
            for d in (2 * step + 2, 2 * step + 1):
                pass_on(ahead(2 * d * side - d))
    relayed = 4 * last_step
    await_bytes(rows_of(slots1, relayed), recv_sem.at[0, 0])
    for d in range(1, 2 * last_step + 1):
        for side in range(2):
            pass_on(ahead((reach + d) * (2 * side - 1)))
    await_bytes(rows_of(slots1, 6), cross_sem.at[1])
    await_bytes(rows_of(slotsg, 2 * reach - 1), recv_sem.at[0, 1])
    await_bytes(rows_of(slotsg, chips), cross_sem.at[0])

    def gained(c, s):
        h = slots1[c, s].astype(F32)
        g = slotsg[c, s].astype(F32)
        return h, h * jnp.where(upper, g[0:1, :], g[1:2, :])

    def statistics(c, carry):
        def body(s, carry):
            squares, peak = carry
            h, hg = gained(c, s)
            return squares + h * h, jnp.maximum(peak, jnp.abs(hg))

        return lax.fori_loop(0, chips, body, carry, unroll=8)

    carry = statistics(core, (zero, zero))
    passed = 2 * reach + 1 + relayed
    await_bytes(rows_of(slots1, passed), swap_recv.at[0])
    squares, peak = statistics(other, carry)
    swaps = []
    squares = squares + half_turn(squares)
    peak = jnp.maximum(peak, half_turn(peak))
    width = w_qkv.shape[1]
    squares = jnp.broadcast_to(jnp.sum(squares, axis=1, keepdims=True), (8, HEAD))
    peak = jnp.broadcast_to(jnp.max(peak, axis=1, keepdims=True), (8, HEAD))
    rstd = lax.rsqrt(squares / width + 1e-05)
    scale = (peak * rstd + 1e-06) / 448.0
    for b in range(4):
        scale_ref[b] = scale[b, 0]

    share = width // (2 * chips)
    for c in range(2):
        for s in range(chips):
            _, hg = gained(c, s)
            quant = (hg * rstd) / scale
            at = (2 * s + c) * share
            x_ref[:, at : at + share] = jnp.concatenate([quant, half_turn(quant)], axis=1).astype(BF16)
    loads[5].wait()
    columns = w_qkv.shape[0]
    proj = lax.dot_general(
        x_ref[...], w_qkv[...], (((1,), (1,)), ((), ())), preferred_element_type=F32
    )
    proj_ref[...] = jnp.zeros((8, 2 * HEAD), F32)
    proj_ref[:, :columns] = proj * scale[:, 0:1]
    wide = proj_ref[...]
    turn = lax.rem(me, 8)
    turned = wide
    for k in range(1, 8):
        turned = jnp.where(turn == k, pltpu.roll(wide, 16 * k, 1), turned)
    piece = jnp.where(upper, turned[:, :HEAD], half_turn(turned[:, HEAD:])).astype(BF16)
    mine2[...] = piece
    slots2[core, chip] = piece
    half = chips // 2
    far = half - chips // 8
    own2 = slots2.at[core, chip]
    for d in range(half, far, -1):
        for side in range(1 if d == half else 2):
            target = ahead(d - 2 * d * side)
            for c in (core, other):
                remote(mine2, own2, send_sem.at[1, 1], recv_sem.at[1, 1], same_core(target, c))
    for d in range(far, 0, -1):
        for side in range(2):
            remote(
                mine2, own2, send_sem.at[1, 0], recv_sem.at[1, 0],
                same_core(ahead(d - 2 * d * side), core),
            )
    remote(mine2, own2, swap_send.at[2], swap_recv.at[2], partner)
    await_bytes(rows_of(slots2, 2 * far), recv_sem.at[1, 0])
    for d in range(1, far + 1):
        for side in range(2):
            block = slots2.at[core, ahead(d - 2 * d * side)]
            remote(block, block, swap_send.at[2], swap_recv.at[2], partner)
    loads[6].wait()
    loads[7].wait()
    beyond = 2 * (half - far) - 1
    await_bytes(rows_of(slots2, 2 * beyond), recv_sem.at[1, 1])
    await_bytes(rows_of(slots2, 2 * far + 1), swap_recv.at[2])

    def arrived2(s):
        return slots2[s % 2, s // 2].astype(F32)

    def halves(h):
        g, k = h // 9, h % 9
        first = arrived2(8 * g + k) if k < 8 else None
        second = arrived2(8 * g + k - 1) if k > 0 else None
        return first, second

    def pair(p):
        a0, b0 = halves(2 * p)
        a1, b1 = halves(2 * p + 1)
        low = (a0 if a0 is not None else zero) + (half_turn(b0) if b0 is not None else zero)
        high = (half_turn(a1) if a1 is not None else zero) + (b1 if b1 is not None else zero)
        return jnp.where(upper, low, high)

    def rotated(value):
        return value * cosine + pltpu.roll(value, HEAD // 2, 1) * sine

    for p in range(QUERY_HEADS // 2):
        q = rotated(pair(p)).astype(BF16)
        q_bf[8 * p : 8 * p + 8, :] = q
        q_f32[8 * p : 8 * p + 8, :] = q.astype(F32)
    base = QUERY_HEADS // 2
    for p in range(2):
        kv_new[8 * p : 8 * p + 8, :] = rotated(pair(base + p))
        kv_new[16 + 8 * p : 24 + 8 * p, :] = pair(base + 2 + p)

    inv = 1.0 / HEAD**0.5
    rows = 64
    row_token = lax.rem(lax.broadcasted_iota(jnp.int32, (rows, HEAD), 0), 4)
    place = me * keys.shape[1] + lax.broadcasted_iota(jnp.int32, (rows, HEAD), 1)
    limit = jnp.zeros((rows, HEAD), jnp.int32)
    for b in range(4):
        limit = jnp.where(row_token == b, lengths_ref[b], limit)
    valid = place < limit
    wide_left = lax.broadcasted_iota(jnp.int32, (rows, HEAD), 1) < HEAD // 2
    even_core = core == 0
    home = me // (QUERY_HEADS // KEY_VALUE_HEADS)
    order = [lax.rem(home + k, KEY_VALUE_HEADS) for k in (2, 1, 3, 0)]

    def attend(k):
        g = order[k]
        q = q_bf[pl.ds(pl.multiple_of(rows * g, rows), rows), :]
        heads = pl.ds(pl.multiple_of(HEAD * g, HEAD), HEAD)
        scores = jnp.zeros((rows, HEAD), F32)
        for b in range(4):
            part = lax.dot_general(
                q, keys[b, :, heads], (((1,), (1,)), ((), ())), preferred_element_type=F32
            )
            scores = jnp.where(row_token == b, part, scores)
        scores = scores * inv
        top = jnp.max(jnp.where(valid, scores, -1e30), axis=1, keepdims=True)
        weights = jnp.where(valid, jnp.exp(scores - top), 0.0)
        total = jnp.sum(weights, axis=1, keepdims=True)
        rounded = weights.astype(BF16)
        block = jnp.zeros((rows, HEAD), F32)
        for b in range(4):
            part = jnp.dot(rounded, values[b, :, heads], preferred_element_type=F32)
            block = jnp.where(row_token == b, part, block)
        stats = jnp.where(wide_left, top, total)
        for j in range(rows // 16):
            for i, value in enumerate((block, stats)):
                one, two = value[16 * j : 16 * j + 8, :], value[16 * j + 8 : 16 * j + 16, :]
                evens = jnp.where(upper, one, half_turn(two))
                odds = jnp.where(upper, half_turn(one), two)
                keep3[4 * k + j, i] = jnp.where(even_core, evens, odds)
                give3[4 * k + j, i] = jnp.where(even_core, odds, evens)
        part = pl.ds(4 * k, 4)
        return swap(give3.at[part], got3.at[part], 3 + k)

    left_half = lane < HEAD // 2

    def both_stats(value):
        turned = pltpu.roll(value, HEAD // 2, 1)
        return jnp.where(left_half, value, turned), jnp.where(left_half, turned, value)

    def settle(k, copy):
        copy.wait_recv()
        for j in range(4):
            at = 4 * k + j
            m0, l0 = both_stats(keep3[at, 1])
            m1, l1 = both_stats(got3[at, 1])
            top = jnp.maximum(m0, m1)
            f0, f1 = jnp.exp(m0 - top), jnp.exp(m1 - top)
            total = l0 * f0 + l1 * f1
            block = keep3[at, 0] * f0 + got3[at, 0] * f1
            stats = zero
            for first, left in ((0, top), (3, total)):
                for i in range(3):
                    bits = left.astype(BF16).astype(F32)
                    stats = jnp.where(lane >= 16 * (first + i), bits, stats)
                    left = left - bits
            stats = jnp.where(lane >= 96, 0.0, stats)
            msg3[2 * at] = jnp.where(upper, block, half_turn(stats)).astype(BF16)
            msg3[2 * at + 1] = jnp.where(upper, half_turn(block), stats).astype(BF16)
        for i in range(8):
            target = 8 * order[k] + i

            def push():
                remote(
                    msg3.at[8 * k + i], slots3.at[chip], send_sem.at[2, 0], recv_sem.at[2, 0],
                    same_core(target, core),
                )

            if k < 3:
                push()
            else:
                pl.when(target != chip)(push)

    copies = []
    for k in range(KEY_VALUE_HEADS):
        copies.append(attend(k))
        if k >= 2:
            settle(k - 2, copies[k - 2])
    settle(2, copies[2])
    settle(3, copies[3])
    slots3[chip] = msg3[24 + lax.rem(chip, 8)]
    swaps.extend(copies)

    def pick(ref, start, index):
        both = ref[pl.ds(pl.multiple_of(start + 8 * (index // 2), 8), 8), :]
        return jnp.where(lax.rem(index, 2) == 1, half_turn(both), both)

    score_new = jnp.sum(pick(q_f32, 0, me) * pick(kv_new, 0, home), axis=1, keepdims=True) * inv
    score_new = jnp.broadcast_to(score_new, (8, HEAD))
    value_new = pick(kv_new, 16, home)

    spot = lax.broadcasted_iota(jnp.int32, (HEAD, 2 * HEAD), 0)
    side = lax.broadcasted_iota(jnp.int32, (HEAD, 2 * HEAD), 1) // HEAD
    chosen = (spot == 48 * side) | (spot == 48 * side + 16) | (spot == 48 * side + 32)
    spread = jnp.where(chosen, 1.0, 0.0).astype(BF16)
    loads[8].wait()
    await_bytes(slots3.at[pl.ds(0, chips - 1)], recv_sem.at[2, 0])
    ml = jnp.dot(slots3[...].reshape(chips * 8, HEAD), spread, preferred_element_type=F32)
    ml = ml.reshape(chips, 8, 2 * HEAD)
    tops = ml[:, :, :HEAD]
    top = half_turn(jnp.max(tops, axis=0))
    summed = zero
    total = zero
    for s in range(chips):
        factor = jnp.exp(half_turn(tops[s]) - top)
        total = total + half_turn(ml[s, :, HEAD:]) * factor
        summed = summed + slots3[s].astype(F32) * factor
    top_new = jnp.maximum(top, score_new)
    keep = jnp.exp(top - top_new)
    fresh = jnp.exp(score_new - top_new)
    total = total * keep + fresh
    summed = summed * keep + fresh * value_new
    att = jnp.where(upper, summed / total, 0.0).astype(BF16)

    per = w_out.shape[1] // (2 * chips)

    def destination(i):
        return ahead(half + ((i + 1) // 2) * (1 - 2 * lax.rem(i, 2)))

    batches, batch = 4, chips // 4
    early = batch

    def expand(side, dest, first):
        for i in range(first, first + batch):
            cols = pl.ds(pl.multiple_of((2 * destination(i) + side) * per, per), per)
            part = jnp.dot(att, w_out[:, cols], preferred_element_type=F32)
            dest[i] = jnp.where(upper, part[:, :HEAD], half_turn(part[:, HEAD:]))

    copies = []
    for k in range(batches):
        expand(other, give4, batch * k)
        part = pl.ds(batch * k, batch)
        copies.append(swap(give4.at[part], got4.at[part], 3 + KEY_VALUE_HEADS + k))
    swaps.extend(copies)
    for k in range(batches):
        expand(core, keep4, batch * k)
    for k in range(batches):
        copies[k].wait_recv()
        indices = range(batch * k, batch * k + batch)
        for i in indices:
            msg4[i] = (keep4[i] + got4[i]).astype(BF16)
        for i in indices:
            if i < chips - 1:
                remote(
                    msg4.at[i], slots4.at[i], send_sem.at[3, 0], recv_sem.at[3, int(i >= early)],
                    same_core(destination(i), core),
                )
    slots4[chips - 1] = msg4[chips - 1]
    await_bytes(slots4.at[pl.ds(0, chips - 1 - early)], recv_sem.at[3, 1])
    sums = [zero] * 4
    for i in range(chips - 1, early - 1, -1):
        sums[i % 4] = sums[i % 4] + slots4[i].astype(F32)
    await_bytes(slots4.at[pl.ds(0, early)], recv_sem.at[3, 0])
    for i in range(early):
        sums[i % 4] = sums[i % 4] + slots4[i].astype(F32)
    result = (sums[0] + sums[1]) + (sums[2] + sums[3])
    out_ref[:, :HEAD] = result[0:4, :].astype(BF16)
    out_ref[:, HEAD:] = half_turn(result)[0:4, :].astype(BF16)

    await_bytes(slots1.at[:, pl.ds(0, 2 * reach + 1)], send_sem.at[0, 0])
    await_bytes(slotsg.at[:, pl.ds(0, chips - 1)], send_sem.at[0, 1])
    await_bytes(mineg, swap_send.at[1])
    await_bytes(rows_of(slots1, passed), swap_send.at[0])
    await_bytes(rows_of(slots2, 2 * far), send_sem.at[1, 0])
    await_bytes(rows_of(slots2, 2 * beyond), send_sem.at[1, 1])
    await_bytes(rows_of(slots2, 2 * far + 1), swap_send.at[2])
    await_bytes(slots3.at[pl.ds(0, chips - 1)], send_sem.at[2, 0])
    await_bytes(slots4.at[pl.ds(0, chips - 1)], send_sem.at[3, 0])
    for copy in swaps:
        copy.wait_send()


def on_device(hidden_in, norm_gain, w_qkv, w_out, key_cache, value_cache, lengths, positions):
    chips = lax.axis_size("tp") // 2
    half = HEAD // 2
    freq = np.float32(500000.0 ** (-(np.arange(half, dtype=np.float64) * 2.0) / HEAD))
    freq = jnp.asarray(np.concatenate([freq, freq])[None, :])
    vmem = pl.BlockSpec(memory_space=pltpu.VMEM)
    smem = pl.BlockSpec(memory_space=pltpu.SMEM)
    anywhere = pl.BlockSpec(memory_space=pl.ANY)
    batch = hidden_in.shape[0]
    tiles = pltpu.VMEM((chips, 8, HEAD), BF16)
    tiles_f32 = pltpu.VMEM((chips, 8, HEAD), F32)
    stats = pltpu.VMEM((chips // 2, 2, 8, HEAD), F32)
    attn_out, token_scale = pl.pallas_call(
        functools.partial(kernel, chips),
        out_shape=(
            jax.ShapeDtypeStruct(hidden_in.shape, BF16),
            jax.ShapeDtypeStruct((batch,), F32),
        ),
        in_specs=[anywhere] * 9,
        out_specs=(vmem, smem),
        scratch_shapes=[
            pltpu.VMEM(w_qkv.shape[::-1], BF16),
            pltpu.VMEM(w_out.shape, BF16),
            pltpu.VMEM(key_cache.shape, BF16),
            pltpu.VMEM(value_cache.shape, BF16),
            pltpu.SMEM(lengths.shape, jnp.int32),
            pltpu.SMEM(positions.shape, jnp.int32),
            pltpu.VMEM(freq.shape, F32),
            pltpu.VMEM(hidden_in.shape, BF16),
            pltpu.VMEM(norm_gain.shape, BF16),
            pltpu.VMEM((8, HEAD), BF16),
            pltpu.VMEM((2, HEAD), BF16),
            pltpu.VMEM((2, chips, 8, HEAD), BF16),
            pltpu.VMEM((2, chips, 2, HEAD), BF16),
            pltpu.VMEM((8, w_qkv.shape[0]), BF16),
            pltpu.VMEM((8, 2 * HEAD), F32),
            pltpu.VMEM((8, HEAD), BF16),
            pltpu.VMEM((2, chips, 8, HEAD), BF16),
            pltpu.VMEM((4 * QUERY_HEADS, HEAD), BF16),
            pltpu.VMEM((4 * QUERY_HEADS, HEAD), F32),
            pltpu.VMEM((32, HEAD), F32),
            stats,
            stats,
            stats,
            tiles,
            tiles,
            tiles_f32,
            tiles_f32,
            tiles_f32,
            tiles,
            tiles,
            pltpu.SemaphoreType.DMA((9,)),
            pltpu.SemaphoreType.DMA((4, 2)),
            pltpu.SemaphoreType.DMA((2, chips // 8, 2)),
            pltpu.SemaphoreType.DMA((2,)),
            pltpu.SemaphoreType.DMA((4, 2)),
            pltpu.SemaphoreType.DMA((7 + KEY_VALUE_HEADS,)),
            pltpu.SemaphoreType.DMA((7 + KEY_VALUE_HEADS,)),
        ],
        compiler_params=pltpu.CompilerParams(collective_id=0, has_side_effects=True),
    )(lengths, positions, freq, hidden_in, norm_gain, w_qkv.T, w_out, key_cache, value_cache)
    return attn_out, token_scale


def solution(mesh):
    placed = (
        P("replica", "tp"),
        P("tp"),
        P(None, "tp"),
        P("tp", None),
        P("replica", "tp", None),
        P("replica", "tp", None),
        P("replica"),
        P("replica"),
    )
    return jax.shard_map(
        on_device,
        mesh=mesh,
        in_specs=placed,
        out_specs=(P("replica", "tp"), P("replica")),
        check_vma=False,
    )
```

```python
import functools

import jax
import jax.numpy as jnp
import numpy as np
from jax import lax
from jax.experimental import pallas as pl
from jax.experimental.pallas import tpu as pltpu
from jax.sharding import PartitionSpec as P

QUERY_HEADS = 64
KEY_VALUE_HEADS = 4
HEAD = 128
MESH = pl.DeviceIdType.MESH
F32 = jnp.float32
BF16 = jnp.bfloat16


def sublane():
    return lax.broadcasted_iota(jnp.int32, (8, HEAD), 0)


def half_turn(value):
    return pltpu.roll(value, 4, 0)


def same_core(index, core):
    return {"tp": 2 * index + core}


def remote(src, dst, send_sem, recv_sem, target):
    copy = pltpu.make_async_remote_copy(
        src_ref=src,
        dst_ref=dst,
        send_sem=send_sem,
        recv_sem=recv_sem,
        device_id=target,
        device_id_type=MESH,
    )
    copy.start()
    return copy


def await_bytes(part, sem):
    pltpu.make_async_copy(part, part, sem).wait()


def kernel(
    chips,
    lengths_hbm, positions_hbm, freq_hbm, hidden_hbm, gain_hbm, w_qkv_hbm, w_out_hbm, key_hbm, value_hbm,
    out_ref, scale_ref,
    w_qkv, w_out, keys, values, lengths_ref, positions_ref, freq_ref, hidden_ref, gain_ref,
    mine1, mineg, slots1, slotsg, proj_ref, mine2, slots2, q_bf, q_f32, kv_new,
    keep3, give3, got3, msg3, slots3, keep4, give4, got4, msg4, slots4,
    load_sem, send_sem, near_sem, recv_sem, swap_send, swap_recv,
):
    me = lax.axis_index("tp")
    chip, core = me // 2, lax.rem(me, 2)
    other = 1 - core
    partner = {"tp": me + 1 - 2 * core}
    reach = chips // 4

    def ahead(d):
        return lax.rem(chip + d + chips, chips)

    barrier = pltpu.get_barrier_semaphore()
    for d in range(reach, 0, -1):
        for target in (ahead(d), ahead(-d)):
            pl.semaphore_signal(
                barrier, inc=1, device_id=same_core(target, core), device_id_type=MESH
            )
    pl.semaphore_signal(barrier, inc=1, device_id=partner, device_id_type=MESH)

    loads = [
        pltpu.make_async_copy(src, dst, load_sem.at[k])
        for k, (src, dst) in enumerate((
            (hidden_hbm, hidden_ref), (gain_hbm, gain_ref), (freq_hbm, freq_ref),
            (positions_hbm, positions_ref), (lengths_hbm, lengths_ref),
            (w_qkv_hbm, w_qkv), (key_hbm, keys), (value_hbm, values), (w_out_hbm, w_out),
        ))
    ]
    for load in loads:
        load.start()

    def swap(src, dst, k):
        return remote(src, dst, swap_send.at[k], swap_recv.at[k], partner)

    sub = sublane()
    upper = sub < 4
    lane = lax.broadcasted_iota(jnp.int32, (8, HEAD), 1)
    token = lax.rem(sub, 4)
    zero = jnp.zeros((8, HEAD), F32)

    loads[0].wait()
    hidden = hidden_ref[...].astype(F32)
    packed = jnp.concatenate([hidden[:, :HEAD], hidden[:, HEAD:]], axis=0).astype(BF16)
    mine1[...] = packed
    slots1[core, chip] = packed
    loads[1].wait()
    gain2 = gain_ref[...].reshape(2, HEAD)
    mineg[...] = gain2
    slotsg[core, chip] = gain2

    pl.semaphore_wait(barrier, 2 * reach + 1)

    parts = ((slots1, mine1), (slotsg, mineg))

    def pace(d):
        return (d - 1) // 2

    for d in range(reach, 0, -1):
        for side in range(2):
            for k, (slots, mine) in enumerate(parts):
                remote(
                    mine, slots.at[core, chip], send_sem.at[0, k], near_sem.at[side, pace(d), k],
                    same_core(ahead(d - 2 * d * side), core),
                )

    loads[2].wait()
    loads[3].wait()
    loads[4].wait()
    position = zero
    for b in range(4):
        position = jnp.where(token == b, positions_ref[b].astype(F32), position)
    angle = position * freq_ref[...]
    cosine = jnp.cos(angle)
    sine = jnp.where(lane < HEAD // 2, -jnp.sin(angle), jnp.sin(angle))

    def rows_of(slots, count):
        return slots.at[0, pl.ds(0, count)]

    for step in range(pace(reach) + 1):
        for side in range(2):
            for k, (slots, _) in enumerate(parts):
                await_bytes(rows_of(slots, 2), near_sem.at[side, step, k])
            for d in (2 * step + 2, 2 * step + 1):
                if d == reach and side == 1:
                    continue
                source = ahead(2 * d * side - d)
                for k, (slots, _) in enumerate(parts):
                    block = slots.at[core, source]
                    remote(
                        block, block, send_sem.at[0, k], recv_sem.at[0, k],
                        same_core(ahead(reach - 2 * reach * side), core),
                    )
    for k, (slots, _) in enumerate(parts):
        await_bytes(rows_of(slots, 2 * reach - 1), recv_sem.at[0, k])
    swaps = [swap(slots1.at[core], slots1.at[core], 0), swap(slotsg.at[core], slotsg.at[core], 1)]

    def gained(c, s):
        h = slots1[c, s].astype(F32)
        g = slotsg[c, s].astype(F32)
        return h, h * jnp.where(upper, g[0:1, :], g[1:2, :])

    def statistics(c, carry):
        def body(s, carry):
            squares, peak = carry
            h, hg = gained(c, s)
            return squares + h * h, jnp.maximum(peak, jnp.abs(hg))

        return lax.fori_loop(0, chips, body, carry, unroll=8)

    carry = statistics(core, (zero, zero))
    for copy in swaps:
        copy.wait_recv()
    squares, peak = statistics(other, carry)
    squares = squares + half_turn(squares)
    peak = jnp.maximum(peak, half_turn(peak))
    width = w_qkv.shape[1]
    squares = jnp.broadcast_to(jnp.sum(squares, axis=1, keepdims=True), (8, HEAD))
    peak = jnp.broadcast_to(jnp.max(peak, axis=1, keepdims=True), (8, HEAD))
    rstd = lax.rsqrt(squares / width + 1e-05)
    scale = (peak * rstd + 1e-06) / 448.0
    scale_ref[...] = scale

    loads[5].wait()
    share = width // (2 * chips)

    def project(s, total):
        for c in range(2):
            _, hg = gained(c, s)
            quant = (hg * rstd) / scale
            x = jnp.concatenate([quant, half_turn(quant)], axis=1).astype(BF16)
            rows = pl.ds(pl.multiple_of((2 * s + c) * share, share), share)
            total = total + lax.dot_general(
                x, w_qkv[:, rows], (((1,), (1,)), ((), ())), preferred_element_type=F32
            )
        return total

    columns = w_qkv.shape[0]
    proj = lax.fori_loop(0, chips, project, jnp.zeros((8, columns), F32), unroll=8)
    proj_ref[...] = jnp.zeros((8, 2 * HEAD), F32)
    proj_ref[:, :columns] = proj * scale[:, 0:1]
    wide = proj_ref[...]
    turn = lax.rem(me, 8)
    turned = wide
    for k in range(1, 8):
        turned = jnp.where(turn == k, pltpu.roll(wide, 16 * k, 1), turned)
    piece = jnp.where(upper, turned[:, :HEAD], half_turn(turned[:, HEAD:])).astype(BF16)
    mine2[...] = piece
    slots2[core, chip] = piece
    half = chips // 2
    own2 = slots2.at[core, chip]
    for d in range(half, 0, -1):
        for side in range(1 if d == half else 2):
            remote(mine2, own2, send_sem.at[1, 0], recv_sem.at[1, 0], same_core(ahead(d - 2 * d * side), core))
    await_bytes(rows_of(slots2, chips - 1), recv_sem.at[1, 0])
    swaps.append(swap(slots2.at[core], slots2.at[core], 2))
    loads[6].wait()
    loads[7].wait()
    await_bytes(slots2.at[0], swap_recv.at[2])

    def arrived2(s):
        return slots2[s % 2, s // 2].astype(F32)

    def halves(h):
        g, k = h // 9, h % 9
        first = arrived2(8 * g + k) if k < 8 else None
        second = arrived2(8 * g + k - 1) if k > 0 else None
        return first, second

    def pair(p):
        a0, b0 = halves(2 * p)
        a1, b1 = halves(2 * p + 1)
        low = (a0 if a0 is not None else zero) + (half_turn(b0) if b0 is not None else zero)
        high = (half_turn(a1) if a1 is not None else zero) + (b1 if b1 is not None else zero)
        return jnp.where(upper, low, high)

    def rotated(value):
        return value * cosine + pltpu.roll(value, HEAD // 2, 1) * sine

    for p in range(QUERY_HEADS // 2):
        q = rotated(pair(p)).astype(BF16)
        q_bf[8 * p : 8 * p + 8, :] = q
        q_f32[8 * p : 8 * p + 8, :] = q.astype(F32)
    base = QUERY_HEADS // 2
    for p in range(2):
        kv_new[8 * p : 8 * p + 8, :] = rotated(pair(base + p))
        kv_new[16 + 8 * p : 24 + 8 * p, :] = pair(base + 2 + p)

    inv = 1.0 / HEAD**0.5
    rows = 64
    row_token = lax.rem(lax.broadcasted_iota(jnp.int32, (rows, HEAD), 0), 4)
    place = me * keys.shape[1] + lax.broadcasted_iota(jnp.int32, (rows, HEAD), 1)
    limit = jnp.zeros((rows, HEAD), jnp.int32)
    for b in range(4):
        limit = jnp.where(row_token == b, lengths_ref[b], limit)
    valid = place < limit
    wide_left = lax.broadcasted_iota(jnp.int32, (rows, HEAD), 1) < HEAD // 2
    even_core = core == 0
    home = me // (QUERY_HEADS // KEY_VALUE_HEADS)
    order = [lax.rem(home + k, KEY_VALUE_HEADS) for k in (2, 1, 3, 0)]

    def attend(k):
        g = order[k]
        q = q_bf[pl.ds(pl.multiple_of(rows * g, rows), rows), :]
        heads = pl.ds(pl.multiple_of(HEAD * g, HEAD), HEAD)
        scores = jnp.zeros((rows, HEAD), F32)
        for b in range(4):
            part = lax.dot_general(
                q, keys[b, :, heads], (((1,), (1,)), ((), ())), preferred_element_type=F32
            )
            scores = jnp.where(row_token == b, part, scores)
        scores = scores * inv
        top = jnp.max(jnp.where(valid, scores, -1e30), axis=1, keepdims=True)
        weights = jnp.where(valid, jnp.exp(scores - top), 0.0)
        total = jnp.sum(weights, axis=1, keepdims=True)
        rounded = weights.astype(BF16)
        block = jnp.zeros((rows, HEAD), F32)
        for b in range(4):
            part = jnp.dot(rounded, values[b, :, heads], preferred_element_type=F32)
            block = jnp.where(row_token == b, part, block)
        stats = jnp.where(wide_left, top, total)
        for j in range(rows // 16):
            for i, value in enumerate((block, stats)):
                one, two = value[16 * j : 16 * j + 8, :], value[16 * j + 8 : 16 * j + 16, :]
                evens = jnp.where(upper, one, half_turn(two))
                odds = jnp.where(upper, half_turn(one), two)
                keep3[4 * k + j, i] = jnp.where(even_core, evens, odds)
                give3[4 * k + j, i] = jnp.where(even_core, odds, evens)
        part = pl.ds(4 * k, 4)
        return swap(give3.at[part], got3.at[part], 3 + k)

    left_half = lane < HEAD // 2

    def both_stats(value):
        turned = pltpu.roll(value, HEAD // 2, 1)
        return jnp.where(left_half, value, turned), jnp.where(left_half, turned, value)

    def settle(k, copy):
        copy.wait_recv()
        for j in range(4):
            at = 4 * k + j
            m0, l0 = both_stats(keep3[at, 1])
            m1, l1 = both_stats(got3[at, 1])
            top = jnp.maximum(m0, m1)
            f0, f1 = jnp.exp(m0 - top), jnp.exp(m1 - top)
            total = l0 * f0 + l1 * f1
            block = keep3[at, 0] * f0 + got3[at, 0] * f1
            stats = zero
            for first, left in ((0, top), (3, total)):
                for i in range(3):
                    bits = left.astype(BF16).astype(F32)
                    stats = jnp.where(lane >= 16 * (first + i), bits, stats)
                    left = left - bits
            stats = jnp.where(lane >= 96, 0.0, stats)
            msg3[2 * at] = jnp.where(upper, block, half_turn(stats)).astype(BF16)
            msg3[2 * at + 1] = jnp.where(upper, half_turn(block), stats).astype(BF16)
        for i in range(8):
            target = 8 * order[k] + i

            def push():
                remote(
                    msg3.at[8 * k + i], slots3.at[chip], send_sem.at[2, 0], recv_sem.at[2, 0],
                    same_core(target, core),
                )

            if k < 3:
                push()
            else:
                pl.when(target != chip)(push)

    copies = []
    for k in range(KEY_VALUE_HEADS):
        copies.append(attend(k))
        if k >= 2:
            settle(k - 2, copies[k - 2])
    settle(2, copies[2])
    settle(3, copies[3])
    slots3[chip] = msg3[24 + lax.rem(chip, 8)]
    swaps.extend(copies)

    def pick(ref, start, index):
        both = ref[pl.ds(pl.multiple_of(start + 8 * (index // 2), 8), 8), :]
        return jnp.where(lax.rem(index, 2) == 1, half_turn(both), both)

    score_new = jnp.sum(pick(q_f32, 0, me) * pick(kv_new, 0, home), axis=1, keepdims=True) * inv
    score_new = jnp.broadcast_to(score_new, (8, HEAD))
    value_new = pick(kv_new, 16, home)

    spot = lax.broadcasted_iota(jnp.int32, (HEAD, 2 * HEAD), 0)
    side = lax.broadcasted_iota(jnp.int32, (HEAD, 2 * HEAD), 1) // HEAD
    chosen = (spot == 48 * side) | (spot == 48 * side + 16) | (spot == 48 * side + 32)
    spread = jnp.where(chosen, 1.0, 0.0).astype(BF16)
    loads[8].wait()
    await_bytes(slots3.at[pl.ds(0, chips - 1)], recv_sem.at[2, 0])
    ml = jnp.dot(slots3[...].reshape(chips * 8, HEAD), spread, preferred_element_type=F32)
    ml = ml.reshape(chips, 8, 2 * HEAD)
    tops = ml[:, :, :HEAD]
    top = half_turn(jnp.max(tops, axis=0))
    summed = zero
    total = zero
    for s in range(chips):
        factor = jnp.exp(half_turn(tops[s]) - top)
        total = total + half_turn(ml[s, :, HEAD:]) * factor
        summed = summed + slots3[s].astype(F32) * factor
    top_new = jnp.maximum(top, score_new)
    keep = jnp.exp(top - top_new)
    fresh = jnp.exp(score_new - top_new)
    total = total * keep + fresh
    summed = summed * keep + fresh * value_new
    att = jnp.where(upper, summed / total, 0.0).astype(BF16)

    per = w_out.shape[1] // (2 * chips)

    def destination(i):
        return ahead(half + ((i + 1) // 2) * (1 - 2 * lax.rem(i, 2)))

    batches, batch = 4, chips // 4

    def expand(side, dest, first):
        for i in range(first, first + batch):
            cols = pl.ds(pl.multiple_of((2 * destination(i) + side) * per, per), per)
            part = jnp.dot(att, w_out[:, cols], preferred_element_type=F32)
            dest[i] = jnp.where(upper, part[:, :HEAD], half_turn(part[:, HEAD:]))

    copies = []
    for k in range(batches):
        expand(other, give4, batch * k)
        part = pl.ds(batch * k, batch)
        copies.append(swap(give4.at[part], got4.at[part], 3 + KEY_VALUE_HEADS + k))
    swaps.extend(copies)
    for k in range(batches):
        expand(core, keep4, batch * k)
    for k in range(batches):
        copies[k].wait_recv()
        indices = range(batch * k, batch * k + batch)
        for i in indices:
            msg4[i] = (keep4[i] + got4[i]).astype(BF16)
        for i in indices:
            if i < chips - 1:
                remote(
                    msg4.at[i], slots4.at[chip], send_sem.at[3, 0], recv_sem.at[3, 0],
                    same_core(destination(i), core),
                )
    slots4[chip] = msg4[chips - 1]
    await_bytes(slots4.at[pl.ds(0, chips - 1)], recv_sem.at[3, 0])

    def gather_sum(s, total):
        return total + slots4[s].astype(F32)

    result = lax.fori_loop(0, chips, gather_sum, zero, unroll=8)
    out_ref[:, :HEAD] = result[0:4, :].astype(BF16)
    out_ref[:, HEAD:] = half_turn(result)[0:4, :].astype(BF16)

    for k, (slots, _) in enumerate(parts):
        await_bytes(rows_of(slots, chips - 1), send_sem.at[0, k])
    await_bytes(rows_of(slots2, chips - 1), send_sem.at[1, 0])
    await_bytes(slots3.at[pl.ds(0, chips - 1)], send_sem.at[2, 0])
    await_bytes(slots4.at[pl.ds(0, chips - 1)], send_sem.at[3, 0])
    for copy in swaps:
        copy.wait_send()


def on_device(hidden_in, norm_gain, w_qkv, w_out, key_cache, value_cache, lengths, positions):
    chips = lax.axis_size("tp") // 2
    half = HEAD // 2
    freq = np.float32(500000.0 ** (-(np.arange(half, dtype=np.float64) * 2.0) / HEAD))
    freq = jnp.asarray(np.concatenate([freq, freq])[None, :])
    vmem = pl.BlockSpec(memory_space=pltpu.VMEM)
    smem = pl.BlockSpec(memory_space=pltpu.SMEM)
    anywhere = pl.BlockSpec(memory_space=pl.ANY)
    batch = hidden_in.shape[0]
    tiles = pltpu.VMEM((chips, 8, HEAD), BF16)
    tiles_f32 = pltpu.VMEM((chips, 8, HEAD), F32)
    stats = pltpu.VMEM((chips // 2, 2, 8, HEAD), F32)
    attn_out, token_scale = pl.pallas_call(
        functools.partial(kernel, chips),
        out_shape=(
            pltpu.VMEM(hidden_in.shape, BF16),
            pltpu.VMEM((8, HEAD), F32),
        ),
        in_specs=[anywhere] * 9,
        out_specs=(vmem, vmem),
        scratch_shapes=[
            pltpu.VMEM(w_qkv.shape[::-1], BF16),
            pltpu.VMEM(w_out.shape, BF16),
            pltpu.VMEM(key_cache.shape, BF16),
            pltpu.VMEM(value_cache.shape, BF16),
            pltpu.SMEM(lengths.shape, jnp.int32),
            pltpu.SMEM(positions.shape, jnp.int32),
            pltpu.VMEM(freq.shape, F32),
            pltpu.VMEM(hidden_in.shape, BF16),
            pltpu.VMEM(norm_gain.shape, BF16),
            pltpu.VMEM((8, HEAD), BF16),
            pltpu.VMEM((2, HEAD), BF16),
            pltpu.VMEM((2, chips, 8, HEAD), BF16),
            pltpu.VMEM((2, chips, 2, HEAD), BF16),
            pltpu.VMEM((8, 2 * HEAD), F32),
            pltpu.VMEM((8, HEAD), BF16),
            pltpu.VMEM((2, chips, 8, HEAD), BF16),
            pltpu.VMEM((4 * QUERY_HEADS, HEAD), BF16),
            pltpu.VMEM((4 * QUERY_HEADS, HEAD), F32),
            pltpu.VMEM((32, HEAD), F32),
            stats,
            stats,
            stats,
            tiles,
            tiles,
            tiles_f32,
            tiles_f32,
            tiles_f32,
            tiles,
            tiles,
            pltpu.SemaphoreType.DMA((9,)),
            pltpu.SemaphoreType.DMA((4, 2)),
            pltpu.SemaphoreType.DMA((2, chips // 8, 2)),
            pltpu.SemaphoreType.DMA((4, 2)),
            pltpu.SemaphoreType.DMA((7 + KEY_VALUE_HEADS,)),
            pltpu.SemaphoreType.DMA((7 + KEY_VALUE_HEADS,)),
        ],
        compiler_params=pltpu.CompilerParams(collective_id=0, has_side_effects=True),
    )(lengths, positions, freq, hidden_in, norm_gain, w_qkv.T, w_out, key_cache, value_cache)
    return attn_out, token_scale[:batch, 0]


def solution(mesh):
    placed = (
        P("replica", "tp"),
        P("tp"),
        P(None, "tp"),
        P("tp", None),
        P("replica", "tp", None),
        P("replica", "tp", None),
        P("replica"),
        P("replica"),
    )
    return jax.shard_map(
        on_device,
        mesh=mesh,
        in_specs=placed,
        out_specs=(P("replica", "tp"), P("replica")),
        check_vma=False,
    )
```

```python
import functools

import jax
import jax.numpy as jnp
import numpy as np
from jax import lax
from jax.experimental import pallas as pl
from jax.experimental.pallas import tpu as pltpu
from jax.sharding import PartitionSpec as P

QUERY_HEADS = 64
KEY_VALUE_HEADS = 4
HEAD = 128
MESH = pl.DeviceIdType.MESH
F32 = jnp.float32
BF16 = jnp.bfloat16


def sublane():
    return lax.broadcasted_iota(jnp.int32, (8, HEAD), 0)


def half_turn(value):
    return pltpu.roll(value, 4, 0)


def same_core(index, core):
    return {"tp": 2 * index + core}


def remote(src, dst, send_sem, recv_sem, target):
    copy = pltpu.make_async_remote_copy(
        src_ref=src,
        dst_ref=dst,
        send_sem=send_sem,
        recv_sem=recv_sem,
        device_id=target,
        device_id_type=MESH,
    )
    copy.start()
    return copy


def await_bytes(part, sem):
    pltpu.make_async_copy(part, part, sem).wait()


def kernel(
    chips,
    lengths_hbm, positions_hbm, freq_hbm, hidden_hbm, gain_hbm, w_qkv_hbm, w_out_hbm, key_hbm, value_hbm,
    out_ref, scale_ref,
    w_qkv, w_out, keys, values, lengths_ref, positions_ref, freq_ref, hidden_ref, gain_ref,
    mine1, mineg, slots1, slotsg, proj_ref, mine2, slots2, q_bf, q_f32,
    msg3, slots3, keep4, give4, got4, msg4, slots4,
    load_sem, send_sem, near_sem, recv_sem, swap_send, swap_recv,
):
    me = lax.axis_index("tp")
    chip, core = me // 2, lax.rem(me, 2)
    other = 1 - core
    partner = {"tp": me + 1 - 2 * core}
    reach = chips // 4

    def ahead(d):
        return lax.rem(chip + d + chips, chips)

    barrier = pltpu.get_barrier_semaphore()
    for d in range(reach, 0, -1):
        for target in (ahead(d), ahead(-d)):
            pl.semaphore_signal(
                barrier, inc=1, device_id=same_core(target, core), device_id_type=MESH
            )
    pl.semaphore_signal(barrier, inc=1, device_id=partner, device_id_type=MESH)

    loads = [
        pltpu.make_async_copy(src, dst, load_sem.at[k])
        for k, (src, dst) in enumerate((
            (hidden_hbm, hidden_ref), (gain_hbm, gain_ref), (freq_hbm, freq_ref),
            (positions_hbm, positions_ref), (lengths_hbm, lengths_ref),
            (w_qkv_hbm, w_qkv), (key_hbm, keys.at[core]), (value_hbm, values.at[core]), (w_out_hbm, w_out),
        ))
    ]
    for load in loads:
        load.start()

    def swap(src, dst, k):
        return remote(src, dst, swap_send.at[k], swap_recv.at[k], partner)

    sub = sublane()
    upper = sub < 4
    lane = lax.broadcasted_iota(jnp.int32, (8, HEAD), 1)
    token = lax.rem(sub, 4)
    zero = jnp.zeros((8, HEAD), F32)

    loads[0].wait()
    hidden = hidden_ref[...].astype(F32)
    packed = jnp.concatenate([hidden[:, :HEAD], hidden[:, HEAD:]], axis=0).astype(BF16)
    mine1[...] = packed
    slots1[core, chip] = packed
    loads[1].wait()
    gain2 = gain_ref[...].reshape(2, HEAD)
    mineg[...] = gain2
    slotsg[core, chip] = gain2

    pl.semaphore_wait(barrier, 2 * reach + 1)

    parts = ((slots1, mine1), (slotsg, mineg))

    def pace(d):
        return (d - 1) // 2

    for d in range(reach, 0, -1):
        for side in range(2):
            for k, (slots, mine) in enumerate(parts):
                remote(
                    mine, slots.at[core, chip], send_sem.at[0, k], near_sem.at[side, pace(d), k],
                    same_core(ahead(d - 2 * d * side), core),
                )

    loads[2].wait()
    loads[3].wait()
    loads[4].wait()
    position = zero
    for b in range(4):
        position = jnp.where(token == b, positions_ref[b].astype(F32), position)
    angle = position * freq_ref[...]
    cosine = jnp.cos(angle)
    sine = jnp.where(lane < HEAD // 2, -jnp.sin(angle), jnp.sin(angle))

    def rows_of(slots, count):
        return slots.at[0, pl.ds(0, count)]

    for step in range(pace(reach) + 1):
        for side in range(2):
            for k, (slots, _) in enumerate(parts):
                await_bytes(rows_of(slots, 2), near_sem.at[side, step, k])
            for d in (2 * step + 2, 2 * step + 1):
                if d == reach and side == 1:
                    continue
                source = ahead(2 * d * side - d)
                for k, (slots, _) in enumerate(parts):
                    block = slots.at[core, source]
                    remote(
                        block, block, send_sem.at[0, k], recv_sem.at[0, k],
                        same_core(ahead(reach - 2 * reach * side), core),
                    )
    for k, (slots, _) in enumerate(parts):
        await_bytes(rows_of(slots, 2 * reach - 1), recv_sem.at[0, k])
    swaps = [swap(slots1.at[core], slots1.at[core], 0), swap(slotsg.at[core], slotsg.at[core], 1)]

    def gained(c, s):
        h = slots1[c, s].astype(F32)
        g = slotsg[c, s].astype(F32)
        return h, h * jnp.where(upper, g[0:1, :], g[1:2, :])

    def statistics(c, carry):
        def body(s, carry):
            squares, peak = carry
            h, hg = gained(c, s)
            return squares + h * h, jnp.maximum(peak, jnp.abs(hg))

        return lax.fori_loop(0, chips, body, carry, unroll=8)

    carry = statistics(core, (zero, zero))
    for copy in swaps:
        copy.wait_recv()
    squares, peak = statistics(other, carry)
    squares = squares + half_turn(squares)
    peak = jnp.maximum(peak, half_turn(peak))
    width = w_qkv.shape[1]
    squares = jnp.broadcast_to(jnp.sum(squares, axis=1, keepdims=True), (8, HEAD))
    peak = jnp.broadcast_to(jnp.max(peak, axis=1, keepdims=True), (8, HEAD))
    rstd = lax.rsqrt(squares / width + 1e-05)
    scale = (peak * rstd + 1e-06) / 448.0
    scale_ref[...] = scale

    loads[5].wait()
    share = width // (2 * chips)

    def project(s, total):
        for c in range(2):
            _, hg = gained(c, s)
            quant = (hg * rstd) / scale
            x = jnp.concatenate([quant, half_turn(quant)], axis=1).astype(BF16)
            rows = pl.ds(pl.multiple_of((2 * s + c) * share, share), share)
            total = total + lax.dot_general(
                x, w_qkv[:, rows], (((1,), (1,)), ((), ())), preferred_element_type=F32
            )
        return total

    columns = w_qkv.shape[0]
    proj = lax.fori_loop(0, chips, project, jnp.zeros((8, columns), F32), unroll=8)
    proj_ref[...] = jnp.zeros((8, 2 * HEAD), F32)
    proj_ref[:, :columns] = proj * scale[:, 0:1]
    wide = proj_ref[...]
    turn = lax.rem(me, 8)
    turned = wide
    for k in range(1, 8):
        turned = jnp.where(turn == k, pltpu.roll(wide, 16 * k, 1), turned)
    mine2[0] = turned[0:4, :HEAD].astype(BF16)
    mine2[1] = turned[0:4, HEAD:].astype(BF16)

    half = chips // 2
    home = chip // 8
    first = me + me // 8
    seam = QUERY_HEADS - QUERY_HEADS // 8

    def part_for(target, c):
        by_core = lax.rem(first + c, 2)
        by_group = jnp.where(target // 8 == lax.rem(me - seam + 3, 4), 0, 1)
        return mine2.at[jnp.where(me > seam, by_group, by_core)]

    def send2(d, c):
        target = ahead(d)
        remote(
            part_for(target, c), slots2.at[me], send_sem.at[1, 0],
            recv_sem.at[1, int(abs(d) <= 4)], same_core(target, c),
        )

    for d in range(half, 0, -1):
        for c in range(2):
            send2(d, c)
            if d < half:
                send2(-d, c)
    remote(part_for(chip, other), slots2.at[me], send_sem.at[1, 0], recv_sem.at[1, 1], partner)

    @pl.when(me == seam)
    def _():
        for target in range(8):
            for c in range(2):
                remote(
                    mine2.at[1], slots2.at[2 * chips], send_sem.at[1, 1], recv_sem.at[2, 1],
                    same_core(target, c),
                )

    none = 2 * chips + 1
    slots2[me] = part_for(chip, core)[...]
    slots2[none] = jnp.zeros((4, HEAD), BF16)
    loads[6].wait()
    loads[7].wait()
    await_bytes(slots2.at[pl.ds(0, 17)], recv_sem.at[1, 1])
    swaps.append(swap(keys.at[core], keys.at[core], 2))
    swaps.append(swap(values.at[core], values.at[core], 3))
    await_bytes(slots2.at[pl.ds(0, 2 * chips - 18)], recv_sem.at[1, 0])

    @pl.when(home == 0)
    def _():
        await_bytes(slots2.at[pl.ds(0, 1)], recv_sem.at[2, 1])

    def sources(h):
        g, k = h // 9, h % 9
        return 8 * g + k if k < 8 else none, 8 * g + k - 1 if k > 0 else none

    def joined(a, b):
        return slots2[a].astype(F32) + slots2[b].astype(F32)

    def own_head(i):
        even, odd = sources(2 * i), sources(2 * i + 1)
        return joined(*(e + core * (o - e) for e, o in zip(even, odd)))

    def rotated(value):
        count = value.shape[0]
        return value * cosine[:count] + pltpu.roll(value, HEAD // 2, 1) * sine[:count]

    for p in range(chips // 2):
        q = rotated(jnp.concatenate([own_head(2 * p), own_head(2 * p + 1)], axis=0)).astype(BF16)
        q_bf[8 * p : 8 * p + 8, :] = q
        q_f32[8 * p : 8 * p + 8, :] = q.astype(F32)
    key_new = joined(seam + 1 + home, jnp.where(home == 0, 2 * chips, seam + home))
    key_new = rotated(jnp.concatenate([key_new, key_new], axis=0))
    value_new = joined(jnp.where(home == 3, none, seam + 5 + home), seam + 4 + home)
    value_new = jnp.concatenate([value_new, value_new], axis=0)

    inv = 1.0 / HEAD**0.5
    rows = 32
    row_token = lax.rem(lax.broadcasted_iota(jnp.int32, (rows, HEAD), 0), 4)
    wide_lane = lax.broadcasted_iota(jnp.int32, (rows, HEAD), 1)
    limit = jnp.zeros((rows, HEAD), jnp.int32)
    for b in range(4):
        limit = jnp.where(row_token == b, lengths_ref[b], limit)
    span = keys.shape[2]
    order = [lax.rem(home + k, KEY_VALUE_HEADS) for k in (2, 1, 3, 0)]
    for copy in swaps[2:4]:
        copy.wait_recv()

    def attend(k):
        g = order[k]
        q = q_bf[pl.ds(pl.multiple_of(rows * g, rows), rows), :]
        heads = pl.ds(pl.multiple_of(HEAD * g, HEAD), HEAD)
        found = []
        for c in range(2):
            scores = jnp.zeros((rows, HEAD), F32)
            for b in range(4):
                part = lax.dot_general(
                    q, keys[c, b, :, heads], (((1,), (1,)), ((), ())), preferred_element_type=F32
                )
                scores = jnp.where(row_token == b, part, scores)
            scores = scores * inv
            valid = (2 * chip + c) * span + wide_lane < limit
            top = jnp.max(jnp.where(valid, scores, -1e30), axis=1, keepdims=True)
            weights = jnp.where(valid, jnp.exp(scores - top), 0.0)
            total = jnp.sum(weights, axis=1, keepdims=True)
            rounded = weights.astype(BF16)
            block = jnp.zeros((rows, HEAD), F32)
            for b in range(4):
                part = jnp.dot(rounded, values[c, b, :, heads], preferred_element_type=F32)
                block = jnp.where(row_token == b, part, block)
            found.append((top, total, block))
        (m0, l0, o0), (m1, l1, o1) = found
        top = jnp.maximum(m0, m1)
        f0, f1 = jnp.exp(m0 - top), jnp.exp(m1 - top)
        total = l0 * f0 + l1 * f1
        block = o0 * f0 + o1 * f1
        stats = jnp.zeros((rows, HEAD), F32)
        for at, left in ((0, top), (3, total)):
            for i in range(3):
                bits = left.astype(BF16).astype(F32)
                stats = jnp.where(wide_lane >= 16 * (at + i), bits, stats)
                left = left - bits
        stats = jnp.where(wide_lane >= 96, 0.0, stats)
        for j in range(rows // 8):
            o, t = block[8 * j : 8 * j + 8, :], stats[8 * j : 8 * j + 8, :]
            msg3[8 * k + 2 * j] = jnp.where(upper, o, half_turn(t)).astype(BF16)
            msg3[8 * k + 2 * j + 1] = jnp.where(upper, half_turn(o), t).astype(BF16)
        for i in range(8):
            target = 8 * g + i

            def push():
                remote(
                    msg3.at[8 * k + i], slots3.at[chip], send_sem.at[2, 0], recv_sem.at[2, 0],
                    same_core(target, core),
                )

            if k < 3:
                push()
            else:
                pl.when(target != chip)(push)

    for k in range(KEY_VALUE_HEADS):
        attend(k)
    slots3[chip] = msg3[24 + lax.rem(chip, 8)]

    both = q_f32[pl.ds(pl.multiple_of(8 * (chip // 2), 8), 8), :]
    own_q = jnp.where(lax.rem(chip, 2) == 1, half_turn(both), both)
    score_new = jnp.sum(own_q * key_new, axis=1, keepdims=True) * inv
    score_new = jnp.broadcast_to(score_new, (8, HEAD))

    spot = lax.broadcasted_iota(jnp.int32, (HEAD, 2 * HEAD), 0)
    side = lax.broadcasted_iota(jnp.int32, (HEAD, 2 * HEAD), 1) // HEAD
    chosen = (spot == 48 * side) | (spot == 48 * side + 16) | (spot == 48 * side + 32)
    spread = jnp.where(chosen, 1.0, 0.0).astype(BF16)
    loads[8].wait()
    await_bytes(slots3.at[pl.ds(0, chips - 1)], recv_sem.at[2, 0])
    ml = jnp.dot(slots3[...].reshape(chips * 8, HEAD), spread, preferred_element_type=F32)
    ml = ml.reshape(chips, 8, 2 * HEAD)
    tops = ml[:, :, :HEAD]
    top = half_turn(jnp.max(tops, axis=0))
    summed = zero
    total = zero
    for s in range(chips):
        factor = jnp.exp(half_turn(tops[s]) - top)
        total = total + half_turn(ml[s, :, HEAD:]) * factor
        summed = summed + slots3[s].astype(F32) * factor
    top_new = jnp.maximum(top, score_new)
    keep = jnp.exp(top - top_new)
    fresh = jnp.exp(score_new - top_new)
    total = total * keep + fresh
    summed = summed * keep + fresh * value_new
    att = jnp.where(upper, summed / total, 0.0).astype(BF16)

    per = w_out.shape[1] // (2 * chips)

    def destination(i):
        return ahead(half + ((i + 1) // 2) * (1 - 2 * lax.rem(i, 2)))

    batches, batch = 4, chips // 8

    def expand(offset, dest, first):
        for i in range(first, first + batch):
            target = destination(offset + i)
            cols = pl.ds(pl.multiple_of(2 * per * target, 2 * per), 2 * per)
            part = jnp.dot(att, w_out[:, cols], preferred_element_type=F32)
            for c in range(2):
                low = part[:, per * c : per * c + HEAD]
                high = part[:, per * c + HEAD : per * c + per]
                dest[2 * i + c] = jnp.where(upper, low, half_turn(high))

    copies = []
    for k in range(batches):
        expand(half * core, give4, batch * k)
        part = pl.ds(2 * batch * k, 2 * batch)
        copies.append(swap(give4.at[part], got4.at[part], 4 + k))
    swaps.extend(copies)
    for k in range(batches):
        expand(half * other, keep4, batch * k)
    for k in range(batches):
        copies[k].wait_recv()
        indices = range(2 * batch * k, 2 * batch * k + 2 * batch)
        for i in indices:
            msg4[i] = (keep4[i] + got4[i]).astype(BF16)
        for i in indices:
            place = half * other + i // 2
            if i // 2 < half - 1:
                remote(
                    msg4.at[i], slots4.at[place], send_sem.at[3, 0], recv_sem.at[3, 0],
                    same_core(destination(place), i % 2),
                )

    @pl.when(core == 1)
    def _():
        for i in (chips - 2, chips - 1):
            remote(
                msg4.at[i], slots4.at[half - 1], send_sem.at[3, 1], recv_sem.at[3, 0],
                same_core(destination(half - 1), i % 2),
            )

    @pl.when(core == 0)
    def _():
        remote(
            msg4.at[chips - 1], slots4.at[chips - 1], send_sem.at[3, 1], recv_sem.at[3, 1], partner
        )
        slots4[chips - 1] = msg4[chips - 2]

    await_bytes(slots4.at[pl.ds(0, chips - 1)], recv_sem.at[3, 0])

    @pl.when(core == 1)
    def _():
        await_bytes(slots4.at[pl.ds(0, 1)], recv_sem.at[3, 1])

    def gather_sum(s, total):
        return total + slots4[s].astype(F32)

    result = lax.fori_loop(0, chips, gather_sum, zero, unroll=8)
    out_ref[:, :HEAD] = result[0:4, :].astype(BF16)
    out_ref[:, HEAD:] = half_turn(result)[0:4, :].astype(BF16)

    for k, (slots, _) in enumerate(parts):
        await_bytes(rows_of(slots, chips - 1), send_sem.at[0, k])
    await_bytes(slots2.at[pl.ds(0, 2 * chips - 1)], send_sem.at[1, 0])

    @pl.when(me == seam)
    def _():
        await_bytes(slots2.at[pl.ds(0, 16)], send_sem.at[1, 1])

    await_bytes(slots3.at[pl.ds(0, chips - 1)], send_sem.at[2, 0])
    await_bytes(slots4.at[pl.ds(0, chips - 2)], send_sem.at[3, 0])

    @pl.when(core == 1)
    def _():
        await_bytes(slots4.at[pl.ds(0, 2)], send_sem.at[3, 1])

    @pl.when(core == 0)
    def _():
        await_bytes(slots4.at[pl.ds(0, 1)], send_sem.at[3, 1])

    for copy in swaps:
        copy.wait_send()


def on_device(hidden_in, norm_gain, w_qkv, w_out, key_cache, value_cache, lengths, positions):
    chips = lax.axis_size("tp") // 2
    half = HEAD // 2
    freq = np.float32(500000.0 ** (-(np.arange(half, dtype=np.float64) * 2.0) / HEAD))
    freq = jnp.asarray(np.concatenate([freq, freq])[None, :])
    vmem = pl.BlockSpec(memory_space=pltpu.VMEM)
    smem = pl.BlockSpec(memory_space=pltpu.SMEM)
    anywhere = pl.BlockSpec(memory_space=pl.ANY)
    batch = hidden_in.shape[0]
    tiles = pltpu.VMEM((chips, 8, HEAD), BF16)
    tiles_f32 = pltpu.VMEM((chips, 8, HEAD), F32)
    attn_out, token_scale = pl.pallas_call(
        functools.partial(kernel, chips),
        out_shape=(
            pltpu.VMEM(hidden_in.shape, BF16),
            pltpu.VMEM((8, HEAD), F32),
        ),
        in_specs=[anywhere] * 9,
        out_specs=(vmem, vmem),
        scratch_shapes=[
            pltpu.VMEM(w_qkv.shape[::-1], BF16),
            pltpu.VMEM(w_out.shape, BF16),
            pltpu.VMEM((2, *key_cache.shape), BF16),
            pltpu.VMEM((2, *value_cache.shape), BF16),
            pltpu.SMEM(lengths.shape, jnp.int32),
            pltpu.SMEM(positions.shape, jnp.int32),
            pltpu.VMEM(freq.shape, F32),
            pltpu.VMEM(hidden_in.shape, BF16),
            pltpu.VMEM(norm_gain.shape, BF16),
            pltpu.VMEM((8, HEAD), BF16),
            pltpu.VMEM((2, HEAD), BF16),
            pltpu.VMEM((2, chips, 8, HEAD), BF16),
            pltpu.VMEM((2, chips, 2, HEAD), BF16),
            pltpu.VMEM((8, 2 * HEAD), F32),
            pltpu.VMEM((2, 4, HEAD), BF16),
            pltpu.VMEM((2 * chips + 2, 4, HEAD), BF16),
            pltpu.VMEM((2 * QUERY_HEADS, HEAD), BF16),
            pltpu.VMEM((2 * QUERY_HEADS, HEAD), F32),
            tiles,
            tiles,
            tiles_f32,
            tiles_f32,
            tiles_f32,
            tiles,
            tiles,
            pltpu.SemaphoreType.DMA((9,)),
            pltpu.SemaphoreType.DMA((4, 2)),
            pltpu.SemaphoreType.DMA((2, chips // 8, 2)),
            pltpu.SemaphoreType.DMA((4, 2)),
            pltpu.SemaphoreType.DMA((7 + KEY_VALUE_HEADS,)),
            pltpu.SemaphoreType.DMA((7 + KEY_VALUE_HEADS,)),
        ],
        compiler_params=pltpu.CompilerParams(collective_id=0, has_side_effects=True),
    )(lengths, positions, freq, hidden_in, norm_gain, w_qkv.T, w_out, key_cache, value_cache)
    return attn_out, token_scale[:batch, 0]


def solution(mesh):
    placed = (
        P("replica", "tp"),
        P("tp"),
        P(None, "tp"),
        P("tp", None),
        P("replica", "tp", None),
        P("replica", "tp", None),
        P("replica"),
        P("replica"),
    )
    return jax.shard_map(
        on_device,
        mesh=mesh,
        in_specs=placed,
        out_specs=(P("replica", "tp"), P("replica")),
        check_vma=False,
    )
```

```python
import functools

import jax
import jax.numpy as jnp
import numpy as np
from jax import lax
from jax.experimental import pallas as pl
from jax.experimental.pallas import tpu as pltpu
from jax.sharding import PartitionSpec as P

QUERY_HEADS = 64
KEY_VALUE_HEADS = 4
HEAD = 128
MESH = pl.DeviceIdType.MESH
F32 = jnp.float32
BF16 = jnp.bfloat16


def sublane():
    return lax.broadcasted_iota(jnp.int32, (8, HEAD), 0)


def half_turn(value):
    return pltpu.roll(value, 4, 0)


def same_core(index, core):
    return {"tp": 2 * index + core}


def remote(src, dst, send_sem, recv_sem, target):
    copy = pltpu.make_async_remote_copy(
        src_ref=src,
        dst_ref=dst,
        send_sem=send_sem,
        recv_sem=recv_sem,
        device_id=target,
        device_id_type=MESH,
    )
    copy.start()
    return copy


def await_bytes(part, sem):
    pltpu.make_async_copy(part, part, sem).wait()


def kernel(
    chips,
    lengths_hbm, positions_hbm, freq_hbm, hidden_hbm, gain_hbm, w_qkv_hbm, w_out_hbm, key_hbm, value_hbm,
    out_ref, scale_ref,
    w_qkv, w_out, keys, values, lengths_ref, positions_ref, freq_ref, hidden_ref, gain_ref,
    mine1, mineg, slots1, slotsg, proj_ref, mine2, slots2, q_bf, q_f32,
    msg3, slots3, keep4, give4, got4, msg4, slots4,
    load_sem, send_sem, near_sem, recv_sem, swap_send, swap_recv,
):
    me = lax.axis_index("tp")
    chip, core = me // 2, lax.rem(me, 2)
    other = 1 - core
    partner = {"tp": me + 1 - 2 * core}
    reach = chips // 4

    def ahead(d):
        return lax.rem(chip + d + chips, chips)

    barrier = pltpu.get_barrier_semaphore()
    for d in range(reach, 0, -1):
        for target in (ahead(d), ahead(-d)):
            pl.semaphore_signal(
                barrier, inc=1, device_id=same_core(target, core), device_id_type=MESH
            )
    pl.semaphore_signal(barrier, inc=1, device_id=partner, device_id_type=MESH)

    loads = [
        pltpu.make_async_copy(src, dst, load_sem.at[k])
        for k, (src, dst) in enumerate((
            (hidden_hbm, hidden_ref), (gain_hbm, gain_ref), (freq_hbm, freq_ref),
            (positions_hbm, positions_ref), (lengths_hbm, lengths_ref),
            (w_qkv_hbm, w_qkv), (key_hbm, keys.at[core]), (value_hbm, values.at[core]), (w_out_hbm, w_out),
        ))
    ]
    for load in loads:
        load.start()

    def swap(src, dst, k):
        return remote(src, dst, swap_send.at[k], swap_recv.at[k], partner)

    sub = sublane()
    upper = sub < 4
    lane = lax.broadcasted_iota(jnp.int32, (8, HEAD), 1)
    token = lax.rem(sub, 4)
    zero = jnp.zeros((8, HEAD), F32)

    loads[0].wait()
    hidden = hidden_ref[...].astype(F32)
    packed = jnp.concatenate([hidden[:, :HEAD], hidden[:, HEAD:]], axis=0).astype(BF16)
    mine1[...] = packed
    slots1[core, chip] = packed
    loads[1].wait()
    gain2 = gain_ref[...].reshape(2, HEAD)
    mineg[...] = gain2
    slotsg[core, chip] = gain2

    pl.semaphore_wait(barrier, 2 * reach + 1)

    parts = ((slots1, mine1), (slotsg, mineg))

    def pace(d):
        return (d - 1) // 2

    for d in range(reach, 0, -1):
        for side in range(2):
            for k, (slots, mine) in enumerate(parts):
                remote(
                    mine, slots.at[core, chip], send_sem.at[0, k], near_sem.at[side, pace(d), k],
                    same_core(ahead(d - 2 * d * side), core),
                )

    loads[2].wait()
    loads[3].wait()
    loads[4].wait()
    position = zero
    for b in range(4):
        position = jnp.where(token == b, positions_ref[b].astype(F32), position)
    angle = position * freq_ref[...]
    cosine = jnp.cos(angle)
    sine = jnp.where(lane < HEAD // 2, -jnp.sin(angle), jnp.sin(angle))

    def rows_of(slots, count):
        return slots.at[0, pl.ds(0, count)]

    for step in range(pace(reach) + 1):
        for side in range(2):
            for k, (slots, _) in enumerate(parts):
                await_bytes(rows_of(slots, 2), near_sem.at[side, step, k])
            for d in (2 * step + 2, 2 * step + 1):
                if d == reach and side == 1:
                    continue
                source = ahead(2 * d * side - d)
                for k, (slots, _) in enumerate(parts):
                    block = slots.at[core, source]
                    remote(
                        block, block, send_sem.at[0, k], recv_sem.at[0, k],
                        same_core(ahead(reach - 2 * reach * side), core),
                    )
    for k, (slots, _) in enumerate(parts):
        await_bytes(rows_of(slots, 2 * reach - 1), recv_sem.at[0, k])
    swaps = [swap(slots1.at[core], slots1.at[core], 0), swap(slotsg.at[core], slotsg.at[core], 1)]

    def gained(c, s):
        h = slots1[c, s].astype(F32)
        g = slotsg[c, s].astype(F32)
        return h, h * jnp.where(upper, g[0:1, :], g[1:2, :])

    def statistics(c, carry):
        def body(s, carry):
            squares, peak = carry
            h, hg = gained(c, s)
            return squares + h * h, jnp.maximum(peak, jnp.abs(hg))

        return lax.fori_loop(0, chips, body, carry, unroll=8)

    carry = statistics(core, (zero, zero))
    for copy in swaps:
        copy.wait_recv()
    squares, peak = statistics(other, carry)
    squares = squares + half_turn(squares)
    peak = jnp.maximum(peak, half_turn(peak))
    width = w_qkv.shape[1]
    squares = jnp.broadcast_to(jnp.sum(squares, axis=1, keepdims=True), (8, HEAD))
    peak = jnp.broadcast_to(jnp.max(peak, axis=1, keepdims=True), (8, HEAD))
    rstd = lax.rsqrt(squares / width + 1e-05)
    scale = (peak * rstd + 1e-06) / 448.0
    scale_ref[...] = scale

    loads[5].wait()
    share = width // (2 * chips)

    def project(s, total):
        for c in range(2):
            _, hg = gained(c, s)
            quant = (hg * rstd) / scale
            x = jnp.concatenate([quant, half_turn(quant)], axis=1).astype(BF16)
            rows = pl.ds(pl.multiple_of((2 * s + c) * share, share), share)
            total = total + lax.dot_general(
                x, w_qkv[:, rows], (((1,), (1,)), ((), ())), preferred_element_type=F32
            )
        return total

    columns = w_qkv.shape[0]
    proj = lax.fori_loop(0, chips, project, jnp.zeros((8, columns), F32), unroll=8)
    proj_ref[...] = jnp.zeros((8, 2 * HEAD), F32)
    proj_ref[:, :columns] = proj * scale[:, 0:1]
    wide = proj_ref[...]
    turn = lax.rem(me, 8)
    turned = wide
    for k in range(1, 8):
        turned = jnp.where(turn == k, pltpu.roll(wide, 16 * k, 1), turned)
    mine2[0] = turned[0:4, :HEAD].astype(BF16)
    mine2[1] = turned[0:4, HEAD:].astype(BF16)

    half = chips // 2
    home = chip // 8
    first = me + me // 8
    seam = QUERY_HEADS - QUERY_HEADS // 8

    def part_for(target, c):
        by_core = lax.rem(first + c, 2)
        by_group = jnp.where(target // 8 == lax.rem(me - seam + 3, 4), 0, 1)
        return mine2.at[jnp.where(me > seam, by_group, by_core)]

    def send2(d, c):
        target = ahead(d)
        remote(
            part_for(target, c), slots2.at[me], send_sem.at[1, 0],
            recv_sem.at[1, int(abs(d) <= 4)], same_core(target, c),
        )

    for d in range(half, 0, -1):
        for c in range(2):
            send2(d, c)
            if d < half:
                send2(-d, c)
    remote(part_for(chip, other), slots2.at[me], send_sem.at[1, 0], recv_sem.at[1, 1], partner)

    @pl.when(me == seam)
    def _():
        for target in range(8):
            for c in range(2):
                remote(
                    mine2.at[1], slots2.at[2 * chips], send_sem.at[1, 1], recv_sem.at[2, 1],
                    same_core(target, c),
                )

    none = 2 * chips + 1
    slots2[me] = part_for(chip, core)[...]
    slots2[none] = jnp.zeros((4, HEAD), BF16)
    loads[6].wait()
    loads[7].wait()
    await_bytes(slots2.at[pl.ds(0, 17)], recv_sem.at[1, 1])
    swaps.append(swap(keys.at[core], keys.at[core], 2))
    swaps.append(swap(values.at[core], values.at[core], 3))
    await_bytes(slots2.at[pl.ds(0, 2 * chips - 18)], recv_sem.at[1, 0])

    @pl.when(home == 0)
    def _():
        await_bytes(slots2.at[pl.ds(0, 1)], recv_sem.at[2, 1])

    def sources(h):
        g, k = h // 9, h % 9
        return 8 * g + k if k < 8 else none, 8 * g + k - 1 if k > 0 else none

    def joined(a, b):
        return slots2[a].astype(F32) + slots2[b].astype(F32)

    def own_head(i):
        even, odd = sources(2 * i), sources(2 * i + 1)
        return joined(*(e + core * (o - e) for e, o in zip(even, odd)))

    def rotated(value):
        count = value.shape[0]
        return value * cosine[:count] + pltpu.roll(value, HEAD // 2, 1) * sine[:count]

    for p in range(chips // 2):
        q = rotated(jnp.concatenate([own_head(2 * p), own_head(2 * p + 1)], axis=0)).astype(BF16)
        q_bf[8 * p : 8 * p + 8, :] = q
        q_f32[8 * p : 8 * p + 8, :] = q.astype(F32)
    key_new = joined(seam + 1 + home, jnp.where(home == 0, 2 * chips, seam + home))
    key_new = rotated(jnp.concatenate([key_new, key_new], axis=0))
    value_new = joined(jnp.where(home == 3, none, seam + 5 + home), seam + 4 + home)
    value_new = jnp.concatenate([value_new, value_new], axis=0)

    inv = 1.0 / HEAD**0.5
    rows = 32
    row_token = lax.rem(lax.broadcasted_iota(jnp.int32, (rows, HEAD), 0), 4)
    wide_lane = lax.broadcasted_iota(jnp.int32, (rows, HEAD), 1)
    limit = jnp.zeros((rows, HEAD), jnp.int32)
    for b in range(4):
        limit = jnp.where(row_token == b, lengths_ref[b], limit)
    span = keys.shape[2]
    turn_back = 2 * (lax.rem(chip, 8) // 4)
    order = [lax.rem(home + k, KEY_VALUE_HEADS) for k in (2, 1 + turn_back, 3 - turn_back, 0)]
    for copy in swaps[2:4]:
        copy.wait_recv()

    def attend(k):
        g = order[k]
        q = q_bf[pl.ds(pl.multiple_of(rows * g, rows), rows), :]
        heads = pl.ds(pl.multiple_of(HEAD * g, HEAD), HEAD)
        both = range(2)
        parts = [
            [
                lax.dot_general(
                    q, keys[c, b, :, heads], (((1,), (1,)), ((), ())), preferred_element_type=F32
                )
                for b in range(4)
            ]
            for c in both
        ]
        tops, weighted, totals = [], [], []
        for c in both:
            scores = parts[c][0]
            for b in range(1, 4):
                scores = jnp.where(row_token == b, parts[c][b], scores)
            valid = (2 * chip + c) * span + wide_lane < limit
            scores = jnp.where(valid, scores * inv, -1e30)
            tops.append(jnp.max(scores, axis=1, keepdims=True))
            weighted.append(jnp.where(valid, jnp.exp(scores - tops[c]), 0.0))
        rounded = [weighted[c].astype(BF16) for c in both]
        parts = [
            [jnp.dot(rounded[c], values[c, b, :, heads], preferred_element_type=F32) for b in range(4)]
            for c in both
        ]
        totals = [jnp.sum(weighted[c], axis=1, keepdims=True) for c in both]
        top = jnp.maximum(tops[0], tops[1])
        factors = [jnp.exp(tops[c] - top) for c in both]
        total = totals[0] * factors[0] + totals[1] * factors[1]
        blocks = []
        for c in both:
            block = parts[c][0]
            for b in range(1, 4):
                block = jnp.where(row_token == b, parts[c][b], block)
            blocks.append(block * factors[c])
        block = blocks[0] + blocks[1]
        stats = jnp.zeros((rows, HEAD), F32)
        for at, left in ((0, top), (3, total)):
            for i in range(3):
                bits = left.astype(BF16).astype(F32)
                stats = jnp.where(wide_lane >= 16 * (at + i), bits, stats)
                left = left - bits
        stats = jnp.where(wide_lane >= 96, 0.0, stats)
        for j in range(rows // 8):
            o, t = block[8 * j : 8 * j + 8, :], stats[8 * j : 8 * j + 8, :]
            msg3[8 * k + 2 * j] = jnp.where(upper, o, half_turn(t)).astype(BF16)
            msg3[8 * k + 2 * j + 1] = jnp.where(upper, half_turn(o), t).astype(BF16)
        for i in range(8):
            target = 8 * g + i

            def push():
                remote(
                    msg3.at[8 * k + i], slots3.at[chip], send_sem.at[2, 0], recv_sem.at[2, 0],
                    same_core(target, core),
                )

            if k < 3:
                push()
            else:
                pl.when(target != chip)(push)

    for k in range(KEY_VALUE_HEADS):
        attend(k)
    slots3[chip] = msg3[24 + lax.rem(chip, 8)]

    both = q_f32[pl.ds(pl.multiple_of(8 * (chip // 2), 8), 8), :]
    own_q = jnp.where(lax.rem(chip, 2) == 1, half_turn(both), both)
    score_new = jnp.sum(own_q * key_new, axis=1, keepdims=True) * inv
    score_new = jnp.broadcast_to(score_new, (8, HEAD))

    spot = lax.broadcasted_iota(jnp.int32, (HEAD, 2 * HEAD), 0)
    side = lax.broadcasted_iota(jnp.int32, (HEAD, 2 * HEAD), 1) // HEAD
    chosen = (spot == 48 * side) | (spot == 48 * side + 16) | (spot == 48 * side + 32)
    spread = jnp.where(chosen, 1.0, 0.0).astype(BF16)
    loads[8].wait()
    await_bytes(slots3.at[pl.ds(0, chips - 1)], recv_sem.at[2, 0])
    ml = jnp.dot(slots3[...].reshape(chips * 8, HEAD), spread, preferred_element_type=F32)
    ml = ml.reshape(chips, 8, 2 * HEAD)
    tops = ml[:, :, :HEAD]
    top = half_turn(jnp.max(tops, axis=0))
    summed = zero
    total = zero
    for s in range(chips):
        factor = jnp.exp(half_turn(tops[s]) - top)
        total = total + half_turn(ml[s, :, HEAD:]) * factor
        summed = summed + slots3[s].astype(F32) * factor
    top_new = jnp.maximum(top, score_new)
    keep = jnp.exp(top - top_new)
    fresh = jnp.exp(score_new - top_new)
    total = total * keep + fresh
    summed = summed * keep + fresh * value_new
    att = jnp.where(upper, summed / total, 0.0).astype(BF16)

    per = w_out.shape[1] // (2 * chips)

    def destination(i):
        return ahead(half + ((i + 1) // 2) * (1 - 2 * lax.rem(i, 2)))

    batches, batch = 4, chips // 8

    def expand(offset, dest, first):
        for i in range(first, first + batch):
            target = destination(offset + i)
            cols = pl.ds(pl.multiple_of(2 * per * target, 2 * per), 2 * per)
            part = jnp.dot(att, w_out[:, cols], preferred_element_type=F32)
            for c in range(2):
                low = part[:, per * c : per * c + HEAD]
                high = part[:, per * c + HEAD : per * c + per]
                dest[2 * i + c] = jnp.where(upper, low, half_turn(high))

    copies = []
    for k in range(batches):
        expand(half * core, give4, batch * k)
        part = pl.ds(2 * batch * k, 2 * batch)
        copies.append(swap(give4.at[part], got4.at[part], 4 + k))
    swaps.extend(copies)
    for k in range(batches):
        expand(half * other, keep4, batch * k)
    for k in range(batches):
        copies[k].wait_recv()
        indices = range(2 * batch * k, 2 * batch * k + 2 * batch)
        for i in indices:
            msg4[i] = (keep4[i] + got4[i]).astype(BF16)
        for i in indices:
            place = half * other + i // 2
            if i // 2 < half - 1:
                remote(
                    msg4.at[i], slots4.at[place], send_sem.at[3, 0], recv_sem.at[3, 0],
                    same_core(destination(place), i % 2),
                )

    @pl.when(core == 1)
    def _():
        for i in (chips - 2, chips - 1):
            remote(
                msg4.at[i], slots4.at[half - 1], send_sem.at[3, 1], recv_sem.at[3, 0],
                same_core(destination(half - 1), i % 2),
            )

    @pl.when(core == 0)
    def _():
        remote(
            msg4.at[chips - 1], slots4.at[chips - 1], send_sem.at[3, 1], recv_sem.at[3, 1], partner
        )
        slots4[chips - 1] = msg4[chips - 2]

    await_bytes(slots4.at[pl.ds(0, chips - 1)], recv_sem.at[3, 0])

    @pl.when(core == 1)
    def _():
        await_bytes(slots4.at[pl.ds(0, 1)], recv_sem.at[3, 1])

    def gather_sum(s, total):
        return total + slots4[s].astype(F32)

    result = lax.fori_loop(0, chips, gather_sum, zero, unroll=8)
    out_ref[:, :HEAD] = result[0:4, :].astype(BF16)
    out_ref[:, HEAD:] = half_turn(result)[0:4, :].astype(BF16)

    for k, (slots, _) in enumerate(parts):
        await_bytes(rows_of(slots, chips - 1), send_sem.at[0, k])
    await_bytes(slots2.at[pl.ds(0, 2 * chips - 1)], send_sem.at[1, 0])

    @pl.when(me == seam)
    def _():
        await_bytes(slots2.at[pl.ds(0, 16)], send_sem.at[1, 1])

    await_bytes(slots3.at[pl.ds(0, chips - 1)], send_sem.at[2, 0])
    await_bytes(slots4.at[pl.ds(0, chips - 2)], send_sem.at[3, 0])

    @pl.when(core == 1)
    def _():
        await_bytes(slots4.at[pl.ds(0, 2)], send_sem.at[3, 1])

    @pl.when(core == 0)
    def _():
        await_bytes(slots4.at[pl.ds(0, 1)], send_sem.at[3, 1])

    for copy in swaps:
        copy.wait_send()


def on_device(hidden_in, norm_gain, w_qkv, w_out, key_cache, value_cache, lengths, positions):
    chips = lax.axis_size("tp") // 2
    half = HEAD // 2
    freq = np.float32(500000.0 ** (-(np.arange(half, dtype=np.float64) * 2.0) / HEAD))
    freq = jnp.asarray(np.concatenate([freq, freq])[None, :])
    vmem = pl.BlockSpec(memory_space=pltpu.VMEM)
    smem = pl.BlockSpec(memory_space=pltpu.SMEM)
    anywhere = pl.BlockSpec(memory_space=pl.ANY)
    batch = hidden_in.shape[0]
    tiles = pltpu.VMEM((chips, 8, HEAD), BF16)
    tiles_f32 = pltpu.VMEM((chips, 8, HEAD), F32)
    attn_out, token_scale = pl.pallas_call(
        functools.partial(kernel, chips),
        out_shape=(
            pltpu.VMEM(hidden_in.shape, BF16),
            pltpu.VMEM((8, HEAD), F32),
        ),
        in_specs=[anywhere] * 9,
        out_specs=(vmem, vmem),
        scratch_shapes=[
            pltpu.VMEM(w_qkv.shape[::-1], BF16),
            pltpu.VMEM(w_out.shape, BF16),
            pltpu.VMEM((2, *key_cache.shape), BF16),
            pltpu.VMEM((2, *value_cache.shape), BF16),
            pltpu.SMEM(lengths.shape, jnp.int32),
            pltpu.SMEM(positions.shape, jnp.int32),
            pltpu.VMEM(freq.shape, F32),
            pltpu.VMEM(hidden_in.shape, BF16),
            pltpu.VMEM(norm_gain.shape, BF16),
            pltpu.VMEM((8, HEAD), BF16),
            pltpu.VMEM((2, HEAD), BF16),
            pltpu.VMEM((2, chips, 8, HEAD), BF16),
            pltpu.VMEM((2, chips, 2, HEAD), BF16),
            pltpu.VMEM((8, 2 * HEAD), F32),
            pltpu.VMEM((2, 4, HEAD), BF16),
            pltpu.VMEM((2 * chips + 2, 4, HEAD), BF16),
            pltpu.VMEM((2 * QUERY_HEADS, HEAD), BF16),
            pltpu.VMEM((2 * QUERY_HEADS, HEAD), F32),
            tiles,
            tiles,
            tiles_f32,
            tiles_f32,
            tiles_f32,
            tiles,
            tiles,
            pltpu.SemaphoreType.DMA((9,)),
            pltpu.SemaphoreType.DMA((4, 2)),
            pltpu.SemaphoreType.DMA((2, chips // 8, 2)),
            pltpu.SemaphoreType.DMA((4, 2)),
            pltpu.SemaphoreType.DMA((7 + KEY_VALUE_HEADS,)),
            pltpu.SemaphoreType.DMA((7 + KEY_VALUE_HEADS,)),
        ],
        compiler_params=pltpu.CompilerParams(collective_id=0, has_side_effects=True),
    )(lengths, positions, freq, hidden_in, norm_gain, w_qkv.T, w_out, key_cache, value_cache)
    return attn_out, token_scale[:batch, 0]


def solution(mesh):
    placed = (
        P("replica", "tp"),
        P("tp"),
        P(None, "tp"),
        P("tp", None),
        P("replica", "tp", None),
        P("replica", "tp", None),
        P("replica"),
        P("replica"),
    )
    return jax.shard_map(
        on_device,
        mesh=mesh,
        in_specs=placed,
        out_specs=(P("replica", "tp"), P("replica")),
        check_vma=False,
    )
```

```python
import functools

import jax
import jax.numpy as jnp
import numpy as np
from jax import lax
from jax.experimental import pallas as pl
from jax.experimental.pallas import tpu as pltpu
from jax.sharding import PartitionSpec as P

QUERY_HEADS = 64
KEY_VALUE_HEADS = 4
HEAD = 128
MESH = pl.DeviceIdType.MESH
F32 = jnp.float32
BF16 = jnp.bfloat16


def sublane():
    return lax.broadcasted_iota(jnp.int32, (8, HEAD), 0)


def half_turn(value):
    return pltpu.roll(value, 4, 0)


def same_core(index, core):
    return {"tp": 2 * index + core}


def remote(src, dst, send_sem, recv_sem, target):
    copy = pltpu.make_async_remote_copy(
        src_ref=src,
        dst_ref=dst,
        send_sem=send_sem,
        recv_sem=recv_sem,
        device_id=target,
        device_id_type=MESH,
    )
    copy.start()
    return copy


def await_bytes(part, sem):
    pltpu.make_async_copy(part, part, sem).wait()


def kernel(
    chips,
    lengths_hbm, positions_hbm, freq_hbm, hidden_hbm, gain_hbm, w_qkv_hbm, w_out_hbm, key_hbm, value_hbm,
    out_ref, scale_ref,
    w_qkv, w_out, keys, values, lengths_ref, positions_ref, freq_ref, hidden_ref, gain_ref,
    mine1, mineg, slots1, slotsg, proj_ref, mine2, slots2, q_bf, q_f32,
    msg3, slots3, keep4, give4, got4, msg4, slots4,
    load_sem, send_sem, near_sem, recv_sem, swap_send, swap_recv,
):
    me = lax.axis_index("tp")
    chip, core = me // 2, lax.rem(me, 2)
    other = 1 - core
    partner = {"tp": me + 1 - 2 * core}
    reach = chips // 4

    def ahead(d):
        return lax.rem(chip + d + chips, chips)

    barrier = pltpu.get_barrier_semaphore()
    for d in range(reach, 0, -1):
        for target in (ahead(d), ahead(-d)):
            pl.semaphore_signal(
                barrier, inc=1, device_id=same_core(target, core), device_id_type=MESH
            )
    pl.semaphore_signal(barrier, inc=1, device_id=partner, device_id_type=MESH)

    loads = [
        pltpu.make_async_copy(src, dst, load_sem.at[k])
        for k, (src, dst) in enumerate((
            (hidden_hbm, hidden_ref), (gain_hbm, gain_ref), (freq_hbm, freq_ref),
            (positions_hbm, positions_ref), (lengths_hbm, lengths_ref),
            (w_qkv_hbm, w_qkv), (key_hbm, keys.at[core]), (value_hbm, values.at[core]), (w_out_hbm, w_out),
        ))
    ]
    for load in loads:
        load.start()

    def swap(src, dst, k):
        return remote(src, dst, swap_send.at[k], swap_recv.at[k], partner)

    sub = sublane()
    upper = sub < 4
    lane = lax.broadcasted_iota(jnp.int32, (8, HEAD), 1)
    token = lax.rem(sub, 4)
    zero = jnp.zeros((8, HEAD), F32)

    loads[0].wait()
    hidden = hidden_ref[...].astype(F32)
    packed = jnp.concatenate([hidden[:, :HEAD], hidden[:, HEAD:]], axis=0).astype(BF16)
    mine1[...] = packed
    slots1[core, chip] = packed
    loads[1].wait()
    gain2 = gain_ref[...].reshape(2, HEAD)
    mineg[...] = gain2
    slotsg[core, chip] = gain2

    pl.semaphore_wait(barrier, 2 * reach + 1)

    parts = ((slots1, mine1), (slotsg, mineg))

    def pace(d):
        return (d - 1) // 2

    for d in range(reach, 0, -1):
        for side in range(2):
            for k, (slots, mine) in enumerate(parts):
                remote(
                    mine, slots.at[core, chip], send_sem.at[0, k], near_sem.at[side, pace(d), k],
                    same_core(ahead(d - 2 * d * side), core),
                )

    loads[2].wait()
    loads[3].wait()
    loads[4].wait()
    position = zero
    for b in range(4):
        position = jnp.where(token == b, positions_ref[b].astype(F32), position)
    angle = position * freq_ref[...]
    cosine = jnp.cos(angle)
    sine = jnp.where(lane < HEAD // 2, -jnp.sin(angle), jnp.sin(angle))

    def rows_of(slots, count):
        return slots.at[0, pl.ds(0, count)]

    for step in range(pace(reach) + 1):
        for side in range(2):
            for k, (slots, _) in enumerate(parts):
                await_bytes(rows_of(slots, 2), near_sem.at[side, step, k])
            for d in (2 * step + 2, 2 * step + 1):
                if d == reach and side == 1:
                    continue
                source = ahead(2 * d * side - d)
                for k, (slots, _) in enumerate(parts):
                    block = slots.at[core, source]
                    remote(
                        block, block, send_sem.at[0, k], recv_sem.at[0, k],
                        same_core(ahead(reach - 2 * reach * side), core),
                    )
    for k, (slots, _) in enumerate(parts):
        await_bytes(rows_of(slots, 2 * reach - 1), recv_sem.at[0, k])
    swaps = [swap(slots1.at[core], slots1.at[core], 0), swap(slotsg.at[core], slotsg.at[core], 1)]

    def gained(c, s):
        h = slots1[c, s].astype(F32)
        g = slotsg[c, s].astype(F32)
        return h, h * jnp.where(upper, g[0:1, :], g[1:2, :])

    def statistics(c, carry):
        def body(s, carry):
            squares, peak = carry
            h, hg = gained(c, s)
            return squares + h * h, jnp.maximum(peak, jnp.abs(hg))

        return lax.fori_loop(0, chips, body, carry, unroll=8)

    carry = statistics(core, (zero, zero))
    for copy in swaps:
        copy.wait_recv()
    squares, peak = statistics(other, carry)
    squares = squares + half_turn(squares)
    peak = jnp.maximum(peak, half_turn(peak))
    width = w_qkv.shape[1]
    squares = jnp.broadcast_to(jnp.sum(squares, axis=1, keepdims=True), (8, HEAD))
    peak = jnp.broadcast_to(jnp.max(peak, axis=1, keepdims=True), (8, HEAD))
    rstd = lax.rsqrt(squares / width + 1e-05)
    scale = (peak * rstd + 1e-06) / 448.0
    scale_ref[...] = scale

    loads[5].wait()
    share = width // (2 * chips)

    def project(s, total):
        for c in range(2):
            _, hg = gained(c, s)
            quant = (hg * rstd) / scale
            x = jnp.concatenate([quant, half_turn(quant)], axis=1).astype(BF16)
            rows = pl.ds(pl.multiple_of((2 * s + c) * share, share), share)
            total = total + lax.dot_general(
                x, w_qkv[:, rows], (((1,), (1,)), ((), ())), preferred_element_type=F32
            )
        return total

    columns = w_qkv.shape[0]
    proj = lax.fori_loop(0, chips, project, jnp.zeros((8, columns), F32), unroll=16)
    proj_ref[...] = jnp.zeros((8, 2 * HEAD), F32)
    proj_ref[:, :columns] = proj * scale[:, 0:1]
    wide = proj_ref[...]
    turn = lax.rem(me, 8)
    turned = wide
    for k in range(1, 8):
        turned = jnp.where(turn == k, pltpu.roll(wide, 16 * k, 1), turned)
    mine2[0] = turned[0:4, :HEAD].astype(BF16)
    mine2[1] = turned[0:4, HEAD:].astype(BF16)

    half = chips // 2
    home = chip // 8
    first = me + me // 8
    seam = QUERY_HEADS - QUERY_HEADS // 8

    def part_for(target, c):
        by_core = lax.rem(first + c, 2)
        by_group = jnp.where(target // 8 == lax.rem(me - seam + 3, 4), 0, 1)
        return mine2.at[jnp.where(me > seam, by_group, by_core)]

    def send2(d, c):
        target = ahead(d)
        remote(
            part_for(target, c), slots2.at[me], send_sem.at[1, 0],
            recv_sem.at[1, int(abs(d) <= 4)], same_core(target, c),
        )

    for d in range(half, 0, -1):
        for c in range(2):
            send2(d, c)
            if d < half:
                send2(-d, c)
    remote(part_for(chip, other), slots2.at[me], send_sem.at[1, 0], recv_sem.at[1, 1], partner)

    @pl.when(me == seam)
    def _():
        for target in range(8):
            for c in range(2):
                remote(
                    mine2.at[1], slots2.at[2 * chips], send_sem.at[1, 1], recv_sem.at[2, 1],
                    same_core(target, c),
                )

    none = 2 * chips + 1
    slots2[me] = part_for(chip, core)[...]
    slots2[none] = jnp.zeros((4, HEAD), BF16)
    loads[6].wait()
    loads[7].wait()
    await_bytes(slots2.at[pl.ds(0, 17)], recv_sem.at[1, 1])
    swaps.append(swap(keys.at[core], keys.at[core], 2))
    swaps.append(swap(values.at[core], values.at[core], 3))
    await_bytes(slots2.at[pl.ds(0, 2 * chips - 18)], recv_sem.at[1, 0])

    @pl.when(home == 0)
    def _():
        await_bytes(slots2.at[pl.ds(0, 1)], recv_sem.at[2, 1])

    def sources(h):
        g, k = h // 9, h % 9
        return 8 * g + k if k < 8 else none, 8 * g + k - 1 if k > 0 else none

    def joined(a, b):
        return slots2[a].astype(F32) + slots2[b].astype(F32)

    def own_head(i):
        even, odd = sources(2 * i), sources(2 * i + 1)
        return joined(*(e + core * (o - e) for e, o in zip(even, odd)))

    def rotated(value):
        count = value.shape[0]
        return value * cosine[:count] + pltpu.roll(value, HEAD // 2, 1) * sine[:count]

    for p in range(chips // 2):
        q = rotated(jnp.concatenate([own_head(2 * p), own_head(2 * p + 1)], axis=0)).astype(BF16)
        q_bf[8 * p : 8 * p + 8, :] = q
        q_f32[8 * p : 8 * p + 8, :] = q.astype(F32)
    key_new = joined(seam + 1 + home, jnp.where(home == 0, 2 * chips, seam + home))
    key_new = rotated(jnp.concatenate([key_new, key_new], axis=0))
    value_new = joined(jnp.where(home == 3, none, seam + 5 + home), seam + 4 + home)
    value_new = jnp.concatenate([value_new, value_new], axis=0)

    inv = 1.0 / HEAD**0.5
    rows = 32
    row_token = lax.rem(lax.broadcasted_iota(jnp.int32, (rows, HEAD), 0), 4)
    wide_lane = lax.broadcasted_iota(jnp.int32, (rows, HEAD), 1)
    limit = jnp.zeros((rows, HEAD), jnp.int32)
    for b in range(4):
        limit = jnp.where(row_token == b, lengths_ref[b], limit)
    span = keys.shape[2]
    turn_back = 2 * (lax.rem(chip, 8) // 4)
    order = [lax.rem(home + k, KEY_VALUE_HEADS) for k in (2, 1 + turn_back, 3 - turn_back, 0)]
    for copy in swaps[2:4]:
        copy.wait_recv()

    def attend(k):
        g = order[k]
        q = q_bf[pl.ds(pl.multiple_of(rows * g, rows), rows), :]
        heads = pl.ds(pl.multiple_of(HEAD * g, HEAD), HEAD)
        both = range(2)
        parts = [
            [
                lax.dot_general(
                    q, keys[c, b, :, heads], (((1,), (1,)), ((), ())), preferred_element_type=F32
                )
                for b in range(4)
            ]
            for c in both
        ]
        tops, weighted, totals = [], [], []
        for c in both:
            scores = parts[c][0]
            for b in range(1, 4):
                scores = jnp.where(row_token == b, parts[c][b], scores)
            valid = (2 * chip + c) * span + wide_lane < limit
            scores = jnp.where(valid, scores * inv, -1e30)
            tops.append(jnp.max(scores, axis=1, keepdims=True))
            weighted.append(jnp.where(valid, jnp.exp(scores - tops[c]), 0.0))
        rounded = [weighted[c].astype(BF16) for c in both]
        parts = [
            [jnp.dot(rounded[c], values[c, b, :, heads], preferred_element_type=F32) for b in range(4)]
            for c in both
        ]
        totals = [jnp.sum(weighted[c], axis=1, keepdims=True) for c in both]
        top = jnp.maximum(tops[0], tops[1])
        factors = [jnp.exp(tops[c] - top) for c in both]
        total = totals[0] * factors[0] + totals[1] * factors[1]
        blocks = []
        for c in both:
            block = parts[c][0]
            for b in range(1, 4):
                block = jnp.where(row_token == b, parts[c][b], block)
            blocks.append(block * factors[c])
        block = blocks[0] + blocks[1]
        stats = jnp.zeros((rows, HEAD), F32)
        for at, left in ((0, top), (3, total)):
            for i in range(3):
                bits = left.astype(BF16).astype(F32)
                stats = jnp.where(wide_lane >= 16 * (at + i), bits, stats)
                left = left - bits
        stats = jnp.where(wide_lane >= 96, 0.0, stats)
        for j in range(rows // 8):
            o, t = block[8 * j : 8 * j + 8, :], stats[8 * j : 8 * j + 8, :]
            msg3[8 * k + 2 * j] = jnp.where(upper, o, half_turn(t)).astype(BF16)
            msg3[8 * k + 2 * j + 1] = jnp.where(upper, half_turn(o), t).astype(BF16)
        for i in range(8):
            target = 8 * g + i

            def push():
                remote(
                    msg3.at[8 * k + i], slots3.at[chip], send_sem.at[2, 0], recv_sem.at[2, 0],
                    same_core(target, core),
                )

            if k < 3:
                push()
            else:
                pl.when(target != chip)(push)

    for k in range(KEY_VALUE_HEADS):
        attend(k)
    slots3[chip] = msg3[24 + lax.rem(chip, 8)]

    both = q_f32[pl.ds(pl.multiple_of(8 * (chip // 2), 8), 8), :]
    own_q = jnp.where(lax.rem(chip, 2) == 1, half_turn(both), both)
    score_new = jnp.sum(own_q * key_new, axis=1, keepdims=True) * inv
    score_new = jnp.broadcast_to(score_new, (8, HEAD))

    spot = lax.broadcasted_iota(jnp.int32, (HEAD, 2 * HEAD), 0)
    side = lax.broadcasted_iota(jnp.int32, (HEAD, 2 * HEAD), 1) // HEAD
    chosen = (spot == 48 * side) | (spot == 48 * side + 16) | (spot == 48 * side + 32)
    spread = jnp.where(chosen, 1.0, 0.0).astype(BF16)
    loads[8].wait()
    await_bytes(slots3.at[pl.ds(0, chips - 1)], recv_sem.at[2, 0])
    ml = jnp.dot(slots3[...].reshape(chips * 8, HEAD), spread, preferred_element_type=F32)
    ml = ml.reshape(chips, 8, 2 * HEAD)
    tops = ml[:, :, :HEAD]
    top = half_turn(jnp.max(tops, axis=0))
    summed = zero
    total = zero
    for s in range(chips):
        factor = jnp.exp(half_turn(tops[s]) - top)
        total = total + half_turn(ml[s, :, HEAD:]) * factor
        summed = summed + slots3[s].astype(F32) * factor
    top_new = jnp.maximum(top, score_new)
    keep = jnp.exp(top - top_new)
    fresh = jnp.exp(score_new - top_new)
    total = total * keep + fresh
    summed = summed * keep + fresh * value_new
    att = jnp.where(upper, summed / total, 0.0).astype(BF16)

    per = w_out.shape[1] // (2 * chips)

    def destination(i):
        return ahead(half + ((i + 1) // 2) * (1 - 2 * lax.rem(i, 2)))

    batches, batch = 4, chips // 8

    def expand(offset, dest, first):
        for i in range(first, first + batch):
            target = destination(offset + i)
            cols = pl.ds(pl.multiple_of(2 * per * target, 2 * per), 2 * per)
            part = jnp.dot(att, w_out[:, cols], preferred_element_type=F32)
            for c in range(2):
                low = part[:, per * c : per * c + HEAD]
                high = part[:, per * c + HEAD : per * c + per]
                dest[2 * i + c] = jnp.where(upper, low, half_turn(high))

    copies = []
    for k in range(batches):
        expand(half * core, give4, batch * k)
        part = pl.ds(2 * batch * k, 2 * batch)
        copies.append(swap(give4.at[part], got4.at[part], 4 + k))
    swaps.extend(copies)
    for k in range(batches):
        expand(half * other, keep4, batch * k)
    for k in range(batches):
        copies[k].wait_recv()
        indices = range(2 * batch * k, 2 * batch * k + 2 * batch)
        for i in indices:
            msg4[i] = (keep4[i] + got4[i]).astype(BF16)
        for i in indices:
            place = half * other + i // 2
            if i // 2 < half - 1:
                remote(
                    msg4.at[i], slots4.at[place], send_sem.at[3, 0], recv_sem.at[3, 0],
                    same_core(destination(place), i % 2),
                )

    @pl.when(core == 1)
    def _():
        for i in (chips - 2, chips - 1):
            remote(
                msg4.at[i], slots4.at[half - 1], send_sem.at[3, 1], recv_sem.at[3, 0],
                same_core(destination(half - 1), i % 2),
            )

    @pl.when(core == 0)
    def _():
        remote(
            msg4.at[chips - 1], slots4.at[chips - 1], send_sem.at[3, 1], recv_sem.at[3, 1], partner
        )
        slots4[chips - 1] = msg4[chips - 2]

    await_bytes(slots4.at[pl.ds(0, chips - 1)], recv_sem.at[3, 0])

    @pl.when(core == 1)
    def _():
        await_bytes(slots4.at[pl.ds(0, 1)], recv_sem.at[3, 1])

    def gather_sum(s, total):
        return total + slots4[s].astype(F32)

    result = lax.fori_loop(0, chips, gather_sum, zero, unroll=8)
    out_ref[:, :HEAD] = result[0:4, :].astype(BF16)
    out_ref[:, HEAD:] = half_turn(result)[0:4, :].astype(BF16)

    for k, (slots, _) in enumerate(parts):
        await_bytes(rows_of(slots, chips - 1), send_sem.at[0, k])
    await_bytes(slots2.at[pl.ds(0, 2 * chips - 1)], send_sem.at[1, 0])

    @pl.when(me == seam)
    def _():
        await_bytes(slots2.at[pl.ds(0, 16)], send_sem.at[1, 1])

    await_bytes(slots3.at[pl.ds(0, chips - 1)], send_sem.at[2, 0])
    await_bytes(slots4.at[pl.ds(0, chips - 2)], send_sem.at[3, 0])

    @pl.when(core == 1)
    def _():
        await_bytes(slots4.at[pl.ds(0, 2)], send_sem.at[3, 1])

    @pl.when(core == 0)
    def _():
        await_bytes(slots4.at[pl.ds(0, 1)], send_sem.at[3, 1])

    for copy in swaps:
        copy.wait_send()


def on_device(hidden_in, norm_gain, w_qkv, w_out, key_cache, value_cache, lengths, positions):
    chips = lax.axis_size("tp") // 2
    half = HEAD // 2
    freq = np.float32(500000.0 ** (-(np.arange(half, dtype=np.float64) * 2.0) / HEAD))
    freq = jnp.asarray(np.concatenate([freq, freq])[None, :])
    vmem = pl.BlockSpec(memory_space=pltpu.VMEM)
    smem = pl.BlockSpec(memory_space=pltpu.SMEM)
    anywhere = pl.BlockSpec(memory_space=pl.ANY)
    batch = hidden_in.shape[0]
    tiles = pltpu.VMEM((chips, 8, HEAD), BF16)
    tiles_f32 = pltpu.VMEM((chips, 8, HEAD), F32)
    attn_out, token_scale = pl.pallas_call(
        functools.partial(kernel, chips),
        out_shape=(
            pltpu.VMEM(hidden_in.shape, BF16),
            pltpu.VMEM((8, HEAD), F32),
        ),
        in_specs=[anywhere] * 9,
        out_specs=(vmem, vmem),
        scratch_shapes=[
            pltpu.VMEM(w_qkv.shape[::-1], BF16),
            pltpu.VMEM(w_out.shape, BF16),
            pltpu.VMEM((2, *key_cache.shape), BF16),
            pltpu.VMEM((2, *value_cache.shape), BF16),
            pltpu.SMEM(lengths.shape, jnp.int32),
            pltpu.SMEM(positions.shape, jnp.int32),
            pltpu.VMEM(freq.shape, F32),
            pltpu.VMEM(hidden_in.shape, BF16),
            pltpu.VMEM(norm_gain.shape, BF16),
            pltpu.VMEM((8, HEAD), BF16),
            pltpu.VMEM((2, HEAD), BF16),
            pltpu.VMEM((2, chips, 8, HEAD), BF16),
            pltpu.VMEM((2, chips, 2, HEAD), BF16),
            pltpu.VMEM((8, 2 * HEAD), F32),
            pltpu.VMEM((2, 4, HEAD), BF16),
            pltpu.VMEM((2 * chips + 2, 4, HEAD), BF16),
            pltpu.VMEM((2 * QUERY_HEADS, HEAD), BF16),
            pltpu.VMEM((2 * QUERY_HEADS, HEAD), F32),
            tiles,
            tiles,
            tiles_f32,
            tiles_f32,
            tiles_f32,
            tiles,
            tiles,
            pltpu.SemaphoreType.DMA((9,)),
            pltpu.SemaphoreType.DMA((4, 2)),
            pltpu.SemaphoreType.DMA((2, chips // 8, 2)),
            pltpu.SemaphoreType.DMA((4, 2)),
            pltpu.SemaphoreType.DMA((7 + KEY_VALUE_HEADS,)),
            pltpu.SemaphoreType.DMA((7 + KEY_VALUE_HEADS,)),
        ],
        compiler_params=pltpu.CompilerParams(collective_id=0, has_side_effects=True),
    )(lengths, positions, freq, hidden_in, norm_gain, w_qkv.T, w_out, key_cache, value_cache)
    return attn_out, token_scale[:batch, 0]


def solution(mesh):
    placed = (
        P("replica", "tp"),
        P("tp"),
        P(None, "tp"),
        P("tp", None),
        P("replica", "tp", None),
        P("replica", "tp", None),
        P("replica"),
        P("replica"),
    )
    return jax.shard_map(
        on_device,
        mesh=mesh,
        in_specs=placed,
        out_specs=(P("replica", "tp"), P("replica")),
        check_vma=False,
    )
```

```python
import functools

import jax
import jax.numpy as jnp
import numpy as np
from jax import lax
from jax.experimental import pallas as pl
from jax.experimental.pallas import tpu as pltpu
from jax.sharding import PartitionSpec as P

QUERY_HEADS = 64
KEY_VALUE_HEADS = 4
HEAD = 128
MESH = pl.DeviceIdType.MESH
F32 = jnp.float32
BF16 = jnp.bfloat16


def sublane():
    return lax.broadcasted_iota(jnp.int32, (8, HEAD), 0)


def half_turn(value):
    return pltpu.roll(value, 4, 0)


def same_core(index, core):
    return {"tp": 2 * index + core}


def remote(src, dst, send_sem, recv_sem, target):
    copy = pltpu.make_async_remote_copy(
        src_ref=src,
        dst_ref=dst,
        send_sem=send_sem,
        recv_sem=recv_sem,
        device_id=target,
        device_id_type=MESH,
    )
    copy.start()
    return copy


def await_bytes(part, sem):
    pltpu.make_async_copy(part, part, sem).wait()


def kernel(
    chips,
    lengths_hbm, positions_hbm, freq_hbm, hidden_hbm, gain_hbm, w_qkv_hbm, w_out_hbm, key_hbm, value_hbm,
    out_ref, scale_ref,
    w_qkv, w_out, keys, values, lengths_ref, positions_ref, freq_ref, hidden_ref, gain_ref,
    mine1, mineg, slots1, slotsg, proj_ref, mine2, slots2, q_bf, q_f32,
    msg3, slots3, keep4, give4, got4, msg4, slots4,
    load_sem, send_sem, near_sem, recv_sem, swap_send, swap_recv,
):
    me = lax.axis_index("tp")
    chip, core = me // 2, lax.rem(me, 2)
    other = 1 - core
    partner = {"tp": me + 1 - 2 * core}
    reach = chips // 4

    def ahead(d):
        return lax.rem(chip + d + chips, chips)

    barrier = pltpu.get_barrier_semaphore()
    for d in range(reach, 0, -1):
        for target in (ahead(d), ahead(-d)):
            pl.semaphore_signal(
                barrier, inc=1, device_id=same_core(target, core), device_id_type=MESH
            )
    pl.semaphore_signal(barrier, inc=1, device_id=partner, device_id_type=MESH)

    loads = [
        pltpu.make_async_copy(src, dst, load_sem.at[k])
        for k, (src, dst) in enumerate((
            (hidden_hbm, hidden_ref), (gain_hbm, gain_ref), (freq_hbm, freq_ref),
            (positions_hbm, positions_ref), (lengths_hbm, lengths_ref),
            (w_qkv_hbm, w_qkv), (key_hbm, keys.at[core]), (value_hbm, values.at[core]), (w_out_hbm, w_out),
        ))
    ]
    for load in loads:
        load.start()

    def swap(src, dst, k):
        return remote(src, dst, swap_send.at[k], swap_recv.at[k], partner)

    sub = sublane()
    upper = sub < 4
    lane = lax.broadcasted_iota(jnp.int32, (8, HEAD), 1)
    token = lax.rem(sub, 4)
    zero = jnp.zeros((8, HEAD), F32)

    loads[0].wait()
    hidden = hidden_ref[...].astype(F32)
    packed = jnp.concatenate([hidden[:, :HEAD], hidden[:, HEAD:]], axis=0).astype(BF16)
    mine1[...] = packed
    slots1[core, chip] = packed
    loads[1].wait()
    gain2 = gain_ref[...].reshape(2, HEAD)
    mineg[...] = gain2
    slotsg[core, chip] = gain2

    pl.semaphore_wait(barrier, 2 * reach + 1)

    parts = ((slots1, mine1), (slotsg, mineg))

    def pace(d):
        return (d - 1) // 2

    for d in range(reach, 0, -1):
        for side in range(2):
            for k, (slots, mine) in enumerate(parts):
                remote(
                    mine, slots.at[core, chip], send_sem.at[0, k], near_sem.at[side, pace(d), k],
                    same_core(ahead(d - 2 * d * side), core),
                )

    loads[2].wait()
    loads[3].wait()
    loads[4].wait()
    position = zero
    for b in range(4):
        position = jnp.where(token == b, positions_ref[b].astype(F32), position)
    angle = position * freq_ref[...]
    cosine = jnp.cos(angle)
    sine = jnp.where(lane < HEAD // 2, -jnp.sin(angle), jnp.sin(angle))

    def rows_of(slots, count):
        return slots.at[0, pl.ds(0, count)]

    for step in range(pace(reach) + 1):
        for side in range(2):
            for k, (slots, _) in enumerate(parts):
                await_bytes(rows_of(slots, 2), near_sem.at[side, step, k])
            for d in (2 * step + 2, 2 * step + 1):
                if d == reach and side == 1:
                    continue
                source = ahead(2 * d * side - d)
                for k, (slots, _) in enumerate(parts):
                    block = slots.at[core, source]
                    remote(
                        block, block, send_sem.at[0, k], recv_sem.at[0, k],
                        same_core(ahead(reach - 2 * reach * side), core),
                    )
    for k, (slots, _) in enumerate(parts):
        await_bytes(rows_of(slots, 2 * reach - 1), recv_sem.at[0, k])
    swaps = [swap(slots1.at[core], slots1.at[core], 0), swap(slotsg.at[core], slotsg.at[core], 1)]

    def gained(c, s):
        h = slots1[c, s].astype(F32)
        g = slotsg[c, s].astype(F32)
        return h, h * jnp.where(upper, g[0:1, :], g[1:2, :])

    def statistics(c, carry):
        def body(s, carry):
            squares, peak = carry
            h, hg = gained(c, s)
            return squares + h * h, jnp.maximum(peak, jnp.abs(hg))

        return lax.fori_loop(0, chips, body, carry, unroll=8)

    carry = statistics(core, (zero, zero))
    for copy in swaps:
        copy.wait_recv()
    squares, peak = statistics(other, carry)
    squares = squares + half_turn(squares)
    peak = jnp.maximum(peak, half_turn(peak))
    width = w_qkv.shape[1]
    squares = jnp.broadcast_to(jnp.sum(squares, axis=1, keepdims=True), (8, HEAD))
    peak = jnp.broadcast_to(jnp.max(peak, axis=1, keepdims=True), (8, HEAD))
    rstd = lax.rsqrt(squares / width + 1e-05)
    scale = (peak * rstd + 1e-06) / 448.0
    scale_ref[...] = scale

    loads[5].wait()
    share = width // (2 * chips)

    def project(s, total):
        for c in range(2):
            _, hg = gained(c, s)
            quant = (hg * rstd) / scale
            x = jnp.concatenate([quant, half_turn(quant)], axis=1).astype(BF16)
            rows = pl.ds(pl.multiple_of((2 * s + c) * share, share), share)
            total = total + lax.dot_general(
                x, w_qkv[:, rows], (((1,), (1,)), ((), ())), preferred_element_type=F32
            )
        return total

    columns = w_qkv.shape[0]
    proj = lax.fori_loop(0, chips, project, jnp.zeros((8, columns), F32), unroll=16)
    proj_ref[...] = jnp.zeros((8, 2 * HEAD), F32)
    proj_ref[:, :columns] = proj * scale[:, 0:1]
    wide = proj_ref[...]
    turn = lax.rem(me, 8)
    turned = wide
    for k in range(1, 8):
        turned = jnp.where(turn == k, pltpu.roll(wide, 16 * k, 1), turned)
    mine2[0] = turned[0:4, :HEAD].astype(BF16)
    mine2[1] = turned[0:4, HEAD:].astype(BF16)

    half = chips // 2
    home = chip // 8
    first = me + me // 8
    seam = QUERY_HEADS - QUERY_HEADS // 8

    def part_for(target, c):
        by_core = lax.rem(first + c, 2)
        by_group = jnp.where(target // 8 == lax.rem(me - seam + 3, 4), 0, 1)
        return mine2.at[jnp.where(me > seam, by_group, by_core)]

    def send2(d, c):
        target = ahead(d)
        remote(
            part_for(target, c), slots2.at[me], send_sem.at[1, 0],
            recv_sem.at[1, int(abs(d) <= 4)], same_core(target, c),
        )

    for d in range(half, 0, -1):
        for c in range(2):
            send2(d, c)
            if d < half:
                send2(-d, c)
    remote(part_for(chip, other), slots2.at[me], send_sem.at[1, 0], recv_sem.at[1, 1], partner)

    @pl.when(me == seam)
    def _():
        for target in range(8):
            for c in range(2):
                remote(
                    mine2.at[1], slots2.at[2 * chips], send_sem.at[1, 1], recv_sem.at[2, 1],
                    same_core(target, c),
                )

    none = 2 * chips + 1
    slots2[me] = part_for(chip, core)[...]
    slots2[none] = jnp.zeros((4, HEAD), BF16)
    loads[6].wait()
    loads[7].wait()
    await_bytes(slots2.at[pl.ds(0, 17)], recv_sem.at[1, 1])
    swaps.append(swap(keys.at[core], keys.at[core], 2))
    swaps.append(swap(values.at[core], values.at[core], 3))
    await_bytes(slots2.at[pl.ds(0, 2 * chips - 18)], recv_sem.at[1, 0])

    @pl.when(home == 0)
    def _():
        await_bytes(slots2.at[pl.ds(0, 1)], recv_sem.at[2, 1])

    def sources(h):
        g, k = h // 9, h % 9
        return 8 * g + k if k < 8 else none, 8 * g + k - 1 if k > 0 else none

    def joined(a, b):
        return slots2[a].astype(F32) + slots2[b].astype(F32)

    def own_head(i):
        even, odd = sources(2 * i), sources(2 * i + 1)
        return joined(*(e + core * (o - e) for e, o in zip(even, odd)))

    def rotated(value):
        count = value.shape[0]
        return value * cosine[:count] + pltpu.roll(value, HEAD // 2, 1) * sine[:count]

    for p in range(chips // 2):
        q = rotated(jnp.concatenate([own_head(2 * p), own_head(2 * p + 1)], axis=0)).astype(BF16)
        q_bf[8 * p : 8 * p + 8, :] = q
        q_f32[8 * p : 8 * p + 8, :] = q.astype(F32)
    key_new = joined(seam + 1 + home, jnp.where(home == 0, 2 * chips, seam + home))
    key_new = rotated(jnp.concatenate([key_new, key_new], axis=0))
    value_new = joined(jnp.where(home == 3, none, seam + 5 + home), seam + 4 + home)
    value_new = jnp.concatenate([value_new, value_new], axis=0)

    inv = 1.0 / HEAD**0.5
    rows = 32
    row_token = lax.rem(lax.broadcasted_iota(jnp.int32, (rows, HEAD), 0), 4)
    wide_lane = lax.broadcasted_iota(jnp.int32, (rows, HEAD), 1)
    limit = jnp.zeros((rows, HEAD), jnp.int32)
    for b in range(4):
        limit = jnp.where(row_token == b, lengths_ref[b], limit)
    span = keys.shape[2]
    turn_back = 2 * (lax.rem(chip, 8) // 4)
    order = [lax.rem(home + k, KEY_VALUE_HEADS) for k in (2, 1 + turn_back, 3 - turn_back, 0)]
    for copy in swaps[2:4]:
        copy.wait_recv()

    def attend(k):
        g = order[k]
        q = q_bf[pl.ds(pl.multiple_of(rows * g, rows), rows), :]
        heads = pl.ds(pl.multiple_of(HEAD * g, HEAD), HEAD)
        both = range(2)
        parts = [
            [
                lax.dot_general(
                    q, keys[c, b, :, heads], (((1,), (1,)), ((), ())), preferred_element_type=F32
                )
                for b in range(4)
            ]
            for c in both
        ]
        tops, weighted, totals = [], [], []
        for c in both:
            scores = parts[c][0]
            for b in range(1, 4):
                scores = jnp.where(row_token == b, parts[c][b], scores)
            valid = (2 * chip + c) * span + wide_lane < limit
            scores = jnp.where(valid, scores * inv, -1e30)
            tops.append(jnp.max(scores, axis=1, keepdims=True))
            weighted.append(jnp.where(valid, jnp.exp(scores - tops[c]), 0.0))
        rounded = [weighted[c].astype(BF16) for c in both]
        parts = [
            [jnp.dot(rounded[c], values[c, b, :, heads], preferred_element_type=F32) for b in range(4)]
            for c in both
        ]
        totals = [jnp.sum(weighted[c], axis=1, keepdims=True) for c in both]
        top = jnp.maximum(tops[0], tops[1])
        factors = [jnp.exp(tops[c] - top) for c in both]
        total = totals[0] * factors[0] + totals[1] * factors[1]
        blocks = []
        for c in both:
            block = parts[c][0]
            for b in range(1, 4):
                block = jnp.where(row_token == b, parts[c][b], block)
            blocks.append(block * factors[c])
        block = blocks[0] + blocks[1]
        stats = jnp.zeros((rows, HEAD), F32)
        for at, left in ((0, top), (3, total)):
            for i in range(3):
                bits = left.astype(BF16).astype(F32)
                stats = jnp.where(wide_lane >= 16 * (at + i), bits, stats)
                left = left - bits
        stats = jnp.where(wide_lane >= 96, 0.0, stats)
        for j in range(rows // 8):
            o, t = block[8 * j : 8 * j + 8, :], stats[8 * j : 8 * j + 8, :]
            msg3[8 * k + 2 * j] = jnp.where(upper, o, half_turn(t)).astype(BF16)
            msg3[8 * k + 2 * j + 1] = jnp.where(upper, half_turn(o), t).astype(BF16)
        for i in range(8):
            target = 8 * g + i

            def push():
                remote(
                    msg3.at[8 * k + i], slots3.at[chip], send_sem.at[2, 0], recv_sem.at[2, 0],
                    same_core(target, core),
                )

            if k < 3:
                push()
            else:
                pl.when(target != chip)(push)

    for k in range(KEY_VALUE_HEADS):
        attend(k)
    slots3[chip] = msg3[24 + lax.rem(chip, 8)]

    both = q_f32[pl.ds(pl.multiple_of(8 * (chip // 2), 8), 8), :]
    own_q = jnp.where(lax.rem(chip, 2) == 1, half_turn(both), both)
    score_new = jnp.sum(own_q * key_new, axis=1, keepdims=True) * inv
    score_new = jnp.broadcast_to(score_new, (8, HEAD))

    spot = lax.broadcasted_iota(jnp.int32, (HEAD, 2 * HEAD), 0)
    side = lax.broadcasted_iota(jnp.int32, (HEAD, 2 * HEAD), 1) // HEAD
    chosen = (spot == 48 * side) | (spot == 48 * side + 16) | (spot == 48 * side + 32)
    spread = jnp.where(chosen, 1.0, 0.0).astype(BF16)
    loads[8].wait()
    await_bytes(slots3.at[pl.ds(0, chips - 1)], recv_sem.at[2, 0])
    ml = jnp.dot(slots3[...].reshape(chips * 8, HEAD), spread, preferred_element_type=F32)
    ml = ml.reshape(chips, 8, 2 * HEAD)
    tops = ml[:, :, :HEAD]
    top = half_turn(jnp.max(tops, axis=0))
    summed = zero
    total = zero
    for s in range(chips):
        factor = jnp.exp(half_turn(tops[s]) - top)
        total = total + half_turn(ml[s, :, HEAD:]) * factor
        summed = summed + slots3[s].astype(F32) * factor
    top_new = jnp.maximum(top, score_new)
    keep = jnp.exp(top - top_new)
    fresh = jnp.exp(score_new - top_new)
    total = total * keep + fresh
    summed = summed * keep + fresh * value_new
    att = jnp.where(upper, summed / total, 0.0).astype(BF16)

    per = w_out.shape[1] // (2 * chips)

    def destination(i):
        return ahead(half + ((i + 1) // 2) * (1 - 2 * lax.rem(i, 2)))

    batches, batch = 4, chips // 8

    def expand(offset, dest, first):
        for i in range(first, first + batch):
            target = destination(offset + i)
            cols = pl.ds(pl.multiple_of(2 * per * target, 2 * per), 2 * per)
            part = jnp.dot(att, w_out[:, cols], preferred_element_type=F32)
            for c in range(2):
                low = part[:, per * c : per * c + HEAD]
                high = part[:, per * c + HEAD : per * c + per]
                dest[2 * i + c] = jnp.where(upper, low, half_turn(high))

    copies = []
    for k in range(batches):
        expand(half * core, give4, batch * k)
        part = pl.ds(2 * batch * k, 2 * batch)
        copies.append(swap(give4.at[part], got4.at[part], 4 + k))
    swaps.extend(copies)
    for k in range(batches):
        expand(half * other, keep4, batch * k)
    for k in range(batches):
        copies[k].wait_recv()
        indices = range(2 * batch * k, 2 * batch * k + 2 * batch)
        for i in indices:
            msg4[i] = (keep4[i] + got4[i]).astype(BF16)
        for i in indices:
            place = half * other + i // 2
            if i // 2 < half - 1:
                remote(
                    msg4.at[i], slots4.at[place], send_sem.at[3, 0], recv_sem.at[3, 0],
                    same_core(destination(place), i % 2),
                )

    @pl.when(core == 1)
    def _():
        for i in (chips - 2, chips - 1):
            remote(
                msg4.at[i], slots4.at[half - 1], send_sem.at[3, 1], recv_sem.at[3, 0],
                same_core(destination(half - 1), i % 2),
            )

    @pl.when(core == 0)
    def _():
        remote(
            msg4.at[chips - 1], slots4.at[chips - 1], send_sem.at[3, 1], recv_sem.at[3, 1], partner
        )
        slots4[chips - 1] = msg4[chips - 2]

    await_bytes(slots4.at[pl.ds(0, chips - 1)], recv_sem.at[3, 0])

    @pl.when(core == 1)
    def _():
        await_bytes(slots4.at[pl.ds(0, 1)], recv_sem.at[3, 1])

    def gather_sum(s, sums):
        return tuple(total + slots4[4 * s + j].astype(F32) for j, total in enumerate(sums))

    sums = lax.fori_loop(0, chips // 4, gather_sum, (zero,) * 4, unroll=2)
    result = (sums[0] + sums[1]) + (sums[2] + sums[3])
    out_ref[:, :HEAD] = result[0:4, :].astype(BF16)
    out_ref[:, HEAD:] = half_turn(result)[0:4, :].astype(BF16)

    for k, (slots, _) in enumerate(parts):
        await_bytes(rows_of(slots, chips - 1), send_sem.at[0, k])
    await_bytes(slots2.at[pl.ds(0, 2 * chips - 1)], send_sem.at[1, 0])

    @pl.when(me == seam)
    def _():
        await_bytes(slots2.at[pl.ds(0, 16)], send_sem.at[1, 1])

    await_bytes(slots3.at[pl.ds(0, chips - 1)], send_sem.at[2, 0])
    await_bytes(slots4.at[pl.ds(0, chips - 2)], send_sem.at[3, 0])

    @pl.when(core == 1)
    def _():
        await_bytes(slots4.at[pl.ds(0, 2)], send_sem.at[3, 1])

    @pl.when(core == 0)
    def _():
        await_bytes(slots4.at[pl.ds(0, 1)], send_sem.at[3, 1])

    for copy in swaps:
        copy.wait_send()


def on_device(hidden_in, norm_gain, w_qkv, w_out, key_cache, value_cache, lengths, positions):
    chips = lax.axis_size("tp") // 2
    half = HEAD // 2
    freq = np.float32(500000.0 ** (-(np.arange(half, dtype=np.float64) * 2.0) / HEAD))
    freq = jnp.asarray(np.concatenate([freq, freq])[None, :])
    vmem = pl.BlockSpec(memory_space=pltpu.VMEM)
    smem = pl.BlockSpec(memory_space=pltpu.SMEM)
    anywhere = pl.BlockSpec(memory_space=pl.ANY)
    batch = hidden_in.shape[0]
    tiles = pltpu.VMEM((chips, 8, HEAD), BF16)
    tiles_f32 = pltpu.VMEM((chips, 8, HEAD), F32)
    attn_out, token_scale = pl.pallas_call(
        functools.partial(kernel, chips),
        out_shape=(
            pltpu.VMEM(hidden_in.shape, BF16),
            pltpu.VMEM((8, HEAD), F32),
        ),
        in_specs=[anywhere] * 9,
        out_specs=(vmem, vmem),
        scratch_shapes=[
            pltpu.VMEM(w_qkv.shape[::-1], BF16),
            pltpu.VMEM(w_out.shape, BF16),
            pltpu.VMEM((2, *key_cache.shape), BF16),
            pltpu.VMEM((2, *value_cache.shape), BF16),
            pltpu.SMEM(lengths.shape, jnp.int32),
            pltpu.SMEM(positions.shape, jnp.int32),
            pltpu.VMEM(freq.shape, F32),
            pltpu.VMEM(hidden_in.shape, BF16),
            pltpu.VMEM(norm_gain.shape, BF16),
            pltpu.VMEM((8, HEAD), BF16),
            pltpu.VMEM((2, HEAD), BF16),
            pltpu.VMEM((2, chips, 8, HEAD), BF16),
            pltpu.VMEM((2, chips, 2, HEAD), BF16),
            pltpu.VMEM((8, 2 * HEAD), F32),
            pltpu.VMEM((2, 4, HEAD), BF16),
            pltpu.VMEM((2 * chips + 2, 4, HEAD), BF16),
            pltpu.VMEM((2 * QUERY_HEADS, HEAD), BF16),
            pltpu.VMEM((2 * QUERY_HEADS, HEAD), F32),
            tiles,
            tiles,
            tiles_f32,
            tiles_f32,
            tiles_f32,
            tiles,
            tiles,
            pltpu.SemaphoreType.DMA((9,)),
            pltpu.SemaphoreType.DMA((4, 2)),
            pltpu.SemaphoreType.DMA((2, chips // 8, 2)),
            pltpu.SemaphoreType.DMA((4, 2)),
            pltpu.SemaphoreType.DMA((7 + KEY_VALUE_HEADS,)),
            pltpu.SemaphoreType.DMA((7 + KEY_VALUE_HEADS,)),
        ],
        compiler_params=pltpu.CompilerParams(collective_id=0, has_side_effects=True),
    )(lengths, positions, freq, hidden_in, norm_gain, w_qkv.T, w_out, key_cache, value_cache)
    return attn_out, token_scale[:batch, 0]


def solution(mesh):
    placed = (
        P("replica", "tp"),
        P("tp"),
        P(None, "tp"),
        P("tp", None),
        P("replica", "tp", None),
        P("replica", "tp", None),
        P("replica"),
        P("replica"),
    )
    return jax.shard_map(
        on_device,
        mesh=mesh,
        in_specs=placed,
        out_specs=(P("replica", "tp"), P("replica")),
        check_vma=False,
    )
```
